128 devices in a mesh: row: 64 (over z, y, x), dp: 2 (over core).
Axes of the slice: x: 4, y: 4, z: 4, core: 2. Of those that a mesh axis runs over, the one named last changes fastest.
Arguments:
- x_tok: bfloat16 [131072, 256], P(('dp', 'row'))
- w_up: bfloat16 [256, 1024], replicated
- w_down: bfloat16 [1024, 128], replicated
- item_table: bfloat16 [1048576, 128], P('row')
- cand_ids: int32 [8192], replicated
- log_q: float32 [8192], replicated
- targets: int32 [131072], P(('dp', 'row'))
Outputs:
- output 1: float32 [], replicated
- output 2: float32 [1048576, 128], P('row')
- output 3: float32 [256, 1024], replicated
- output 4: float32 [1024, 128], replicated
All inputs are finite; a program needn't handle non-finite values.
Results may differ from the reference program's by a relative error of at most 0.002604.
Values are sent between devices in bfloat16 or wider.
A program may use at most 1 GiB of HBM per device.

```python
import jax
import jax.numpy as jnp
from jax import lax

D_IN = 256
FFN = 1024
DIM = 128
VOCAB = 1048576
CANDS = 8192
TOKENS = 131072
TOK_BLOCK = 1024


def draw_ids(base_key):
    key_list = jax.random.split(base_key, 6)
    hot_rows = VOCAB // 8
    cold_rows = VOCAB - hot_rows
    half_cands = CANDS // 2
    hot_perm = jax.random.permutation(key_list[0], hot_rows)[:half_cands]
    hot_ids = (hot_perm - hot_perm[0]) % hot_rows
    cold_perm = jax.random.permutation(key_list[1], cold_rows)[:half_cands]
    cold_ids = hot_rows + (cold_perm + (cold_rows - 1 - cold_perm[0])) % cold_rows
    cand_ids = jnp.concatenate([hot_ids, cold_ids]).astype(jnp.int32)
    choice = jax.random.randint(key_list[2], (TOKENS,), 0, 4)
    from_cands = cand_ids[jax.random.randint(key_list[3], (TOKENS,), 0, CANDS)]
    from_hot = jax.random.randint(key_list[4], (TOKENS,), 0, hot_rows)
    from_any = jax.random.randint(key_list[5], (TOKENS,), 0, VOCAB)
    targets = jnp.where(choice == 0, from_cands, jnp.where(choice == 1, from_hot, from_any))
    return cand_ids, targets.astype(jnp.int32)


def setup_inputs(seed: int = 0) -> dict:
    key_list = jax.random.split(jax.random.key(seed), 6)
    x_tok = jax.random.normal(key_list[0], (TOKENS, D_IN), jnp.float32).astype(jnp.bfloat16)
    w_up = (jax.random.normal(key_list[1], (D_IN, FFN), jnp.float32) * D_IN ** -0.5).astype(jnp.bfloat16)
    w_down = (jax.random.normal(key_list[2], (FFN, DIM), jnp.float32) * FFN ** -0.5).astype(jnp.bfloat16)
    item_table = (jax.random.normal(key_list[3], (VOCAB, DIM), jnp.float32) * (1.5 * DIM ** -0.5)).astype(jnp.bfloat16)
    cand_ids, targets = draw_ids(key_list[4])
    log_q = jnp.log(jnp.float32(CANDS)) + jax.random.uniform(key_list[5], (CANDS,), jnp.float32, -3.0, 1.0)
    return {"x_tok": x_tok, "w_up": w_up, "w_down": w_down, "item_table": item_table, "cand_ids": cand_ids, "log_q": log_q, "targets": targets}


def reference(x_tok, w_up, w_down, item_table, cand_ids, log_q, targets):
    cand_rows = item_table[cand_ids]
    n_blocks = TOKENS // TOK_BLOCK
    x_blocks = x_tok.reshape(n_blocks, TOK_BLOCK, D_IN)
    y_blocks = targets.reshape(n_blocks, TOK_BLOCK)

    def block_step(carry, inputs):
        loss_sum, grad_up, grad_down, grad_cand = carry
        x_blk, y_blk = inputs
        pre_act = jnp.dot(x_blk, w_up, preferred_element_type=jnp.float32)
        act_full, gelu_vjp = jax.vjp(jax.nn.gelu, pre_act)
        act_b = act_full.astype(jnp.bfloat16)
        hidden = jnp.dot(act_b, w_down, preferred_element_type=jnp.float32).astype(jnp.bfloat16)
        tgt_rows = item_table[y_blk]
        z_tgt = jnp.sum(hidden.astype(jnp.float32) * tgt_rows.astype(jnp.float32), axis=1)
        z_cand = jnp.dot(hidden, cand_rows.T, preferred_element_type=jnp.float32) - log_q[None, :]
        z_cand = jnp.where(y_blk[:, None] == cand_ids[None, :], -1e9, z_cand)
        row_max = jnp.maximum(z_tgt, jnp.max(z_cand, axis=1))
        e_tgt = jnp.exp(z_tgt - row_max)
        e_cand = jnp.exp(z_cand - row_max[:, None])
        exp_total = e_tgt + jnp.sum(e_cand, axis=1)
        loss_sum = loss_sum + jnp.sum(row_max + jnp.log(exp_total) - z_tgt)
        dz_tgt = (e_tgt / exp_total - 1.0) / TOKENS
        dz_cand = (e_cand / exp_total[:, None] / TOKENS).astype(jnp.bfloat16)
        grad_hid = (dz_tgt[:, None] * tgt_rows.astype(jnp.float32) + jnp.dot(dz_cand, cand_rows, preferred_element_type=jnp.float32)).astype(jnp.bfloat16)
        grad_down = grad_down + jnp.dot(act_b.T, grad_hid, preferred_element_type=jnp.float32)
        grad_act = jnp.dot(grad_hid, w_down.T, preferred_element_type=jnp.float32)
        grad_pre = gelu_vjp(grad_act)[0].astype(jnp.bfloat16)
        grad_up = grad_up + jnp.dot(x_blk.T, grad_pre, preferred_element_type=jnp.float32)
        grad_cand = grad_cand + jnp.dot(dz_cand.T, hidden, preferred_element_type=jnp.float32)
        return (loss_sum, grad_up, grad_down, grad_cand), (dz_tgt, hidden)

    init = (jnp.zeros((), jnp.float32), jnp.zeros((D_IN, FFN), jnp.float32), jnp.zeros((FFN, DIM), jnp.float32), jnp.zeros((CANDS, DIM), jnp.float32))
    (loss_sum, grad_up, grad_down, grad_cand), (dz_blocks, hid_blocks) = lax.scan(block_step, init, (x_blocks, y_blocks))
    dz_flat = dz_blocks.reshape(TOKENS)
    hid_flat = hid_blocks.reshape(TOKENS, DIM).astype(jnp.float32)
    grad_table = jnp.zeros((VOCAB, DIM), jnp.float32).at[cand_ids].add(grad_cand).at[targets].add(dz_flat[:, None] * hid_flat)
    return loss_sum / TOKENS, grad_table, grad_up, grad_down
```

```python
import functools

import jax
import jax.numpy as jnp
from jax import lax
from jax.experimental import pallas as pl
from jax.experimental.pallas import tpu as pltpu
from jax.sharding import PartitionSpec as P

ALL_AXES = ("dp", "row")
MESH = pl.DeviceIdType.MESH
CAP = 128
LANES = 128
ACCS = 2
ANY = pl.BlockSpec(memory_space=pl.ANY)
VMEM = pl.BlockSpec(memory_space=pltpu.VMEM)
SMEM = pl.BlockSpec(memory_space=pltpu.SMEM)


def params():
    return pltpu.CompilerParams(has_side_effects=True, vmem_limit_bytes=60 * 1024 * 1024)


def exchange(n_row, n_dp, both, *xs):
    n_x = len(xs)
    steps = range(n_dp) if both else range(1)
    n_out = n_row * (n_dp if both else 1)

    def kernel(*refs):
        ins, outs = refs[:n_x], refs[n_x:2 * n_x]
        send_sem, recv_sem = refs[2 * n_x:]
        row, dp = lax.axis_index("row"), lax.axis_index("dp")
        slot = dp * n_row + row if both else row
        for i in range(n_x):
            pltpu.make_async_copy(ins[i].at[row], outs[i].at[slot], recv_sem.at[i]).start()

        for e in steps:
            def send(j, carry, e=e):
                peer = lax.rem(row + j, n_row)
                for i in range(n_x):
                    pltpu.make_async_remote_copy(
                        src_ref=ins[i].at[peer],
                        dst_ref=outs[i].at[slot],
                        send_sem=send_sem.at[i, e],
                        recv_sem=recv_sem.at[i],
                        device_id={"row": peer, "dp": lax.rem(dp + e, n_dp)},
                        device_id_type=MESH,
                    ).start()
                return carry
            lax.fori_loop(0 if e else 1, n_row, send, 0)
        for i in range(n_x):
            for e in steps:
                sent = ins[i] if e else ins[i].at[pl.ds(0, n_row - 1)]
                pltpu.make_async_copy(sent, sent, send_sem.at[i, e]).wait()
            pltpu.make_async_copy(outs[i], outs[i], recv_sem.at[i]).wait()

    return pl.pallas_call(
        kernel,
        out_shape=[jax.ShapeDtypeStruct((n_out,) + x.shape[1:], x.dtype) for x in xs],
        in_specs=[VMEM] * n_x,
        out_specs=[VMEM] * n_x,
        scratch_shapes=[pltpu.SemaphoreType.DMA((n_x, n_dp)), pltpu.SemaphoreType.DMA((n_x,))],
        compiler_params=params(),
    )(*xs)


def add_rows(grad, vals, row_ids, counts):
    n_list, width = row_ids.shape
    n_rows = grad.shape[0]
    per_list = vals.shape[0] // n_list

    def kernel(idx, cnt, vals_ref, grad_ref, out_ref, *accs):
        cp_in = pltpu.make_async_copy(grad_ref, accs[0], accs[-1])
        cp_in.start()
        for a in accs[1:-1]:
            a[...] = jnp.zeros_like(a)
        cp_in.wait()

        def one_list(i, carry):
            def group(g, c2):
                for u in range(8):
                    c = g * 8 + u
                    acc = accs[u % ACCS]
                    r = idx[i, c]
                    acc[pl.ds(r, 1), :] += vals_ref[pl.ds(i * per_list + c, 1), :]
                return c2
            return lax.fori_loop(0, (cnt[i] + 7) // 8, group, carry)
        lax.fori_loop(0, n_list, one_list, 0)
        chunk = 512
        rest = n_rows % chunk

        def merge(k, carry):
            sl = pl.ds(pl.multiple_of(k * chunk, chunk), chunk)
            tot = accs[0][sl, :]
            for a in accs[1:-1]:
                tot = tot + a[sl, :]
            accs[0][sl, :] = tot
            return carry
        lax.fori_loop(0, n_rows // chunk, merge, 0)
        if rest:
            sl = pl.ds(n_rows - rest, rest)
            tot = accs[0][sl, :]
            for a in accs[1:-1]:
                tot = tot + a[sl, :]
            accs[0][sl, :] = tot
        cp_out = pltpu.make_async_copy(accs[0], out_ref, accs[-1])
        cp_out.start()
        cp_out.wait()

    return pl.pallas_call(
        kernel,
        out_shape=jax.ShapeDtypeStruct(grad.shape, jnp.float32),
        in_specs=[SMEM, SMEM, VMEM, ANY],
        out_specs=ANY,
        scratch_shapes=[pltpu.VMEM(grad.shape, jnp.float32)] * ACCS + [pltpu.SemaphoreType.DMA],
        compiler_params=pltpu.CompilerParams(vmem_limit_bytes=60 * 1024 * 1024),
    )(row_ids, counts, vals, grad)


def ranks(owner, n_row):
    n = owner.shape[0]
    hot = (owner[:, None] == jnp.arange(n_row)[None, :]).astype(jnp.bfloat16)
    pos = jnp.arange(n)
    before = (pos[:, None] > pos[None, :]).astype(jnp.bfloat16)
    earlier = jnp.dot(before, hot, preferred_element_type=jnp.float32)
    hot32 = hot.astype(jnp.float32)
    return jnp.sum(earlier * hot32, axis=1).astype(jnp.int32), jnp.sum(hot32, axis=0).astype(jnp.int32)


def to_slots(slot, vals, n_slots):
    hit = slot[:, None] == jnp.arange(n_slots)[None, :]
    return [jnp.sum(jnp.where(hit, v[:, None], jnp.zeros((), v.dtype)), axis=0) for v in vals]


def tile_rows(rows, n_row):
    padded = [jnp.pad(r, ((0, 0), (0, LANES - r.shape[1]))) for r in rows]
    padded += [jnp.zeros_like(padded[0])] * (8 - len(rows))
    return jnp.stack(padded, axis=1)


def solution(mesh):
    n_row, n_dp = mesh.shape["row"], mesh.shape["dp"]
    n_dev = n_row * n_dp

    def run_step(x_tok, w_up, w_down, item_table, cand_ids, log_q, targets):
        n_total = x_tok.shape[0]

        def device_step(x_loc, w_up, w_down, tab_loc, cand_ids, log_q, y_loc):
            rows_local, width = tab_loc.shape
            n_tok = y_loc.shape[0]
            n_cand = cand_ids.shape[0]
            row, dp = lax.axis_index("row"), lax.axis_index("dp")
            me = dp * n_row + row
            chunk = n_cand // n_dev
            n_slots = n_row * CAP

            pre_act = jnp.dot(x_loc, w_up, preferred_element_type=jnp.float32)
            act_full, gelu_vjp = jax.vjp(jax.nn.gelu, pre_act)
            act_b = act_full.astype(jnp.bfloat16)
            hidden = jnp.dot(act_b, w_down, preferred_element_type=jnp.float32).astype(jnp.bfloat16)

            my_cands = lax.dynamic_slice_in_dim(cand_ids, me * chunk, chunk)
            ids = jnp.concatenate([y_loc, my_cands])
            owner, local = ids // rows_local, ids % rows_local
            rank, per_owner = ranks(owner, n_row)
            most = jnp.max(per_owner)

            def slots_of(k, rank, owner):
                rel = rank - k * CAP
                return jnp.where((rel >= 0) & (rel < CAP), owner * CAP + rel, n_slots)

            def fetch_round(carry):
                k, _, got = carry
                slot = slots_of(k, rank, owner)
                (want,) = to_slots(slot, [local], n_slots)
                msg = tile_rows([want.reshape(n_row, CAP), jnp.full((n_row, LANES), most, jnp.int32)], n_row)
                (asked,) = exchange(n_row, n_dp, True, msg)
                most_all = jnp.max(asked[:, 1, 0])
                mine = lax.dynamic_slice_in_dim(asked, dp * n_row, n_row)[:, 0, :CAP]
                rows_out = jnp.take(tab_loc, mine, axis=0, mode="clip")
                (rows_in,) = exchange(n_row, n_dp, False, rows_out)
                new = jnp.take(rows_in.reshape(n_slots, width), slot, axis=0, mode="clip")
                return k + 1, most_all, jnp.where((slot < n_slots)[:, None], new, got)

            _, most_all, got = lax.while_loop(
                lambda c: (c[0] == 0) | (c[0] * CAP < c[1]),
                fetch_round,
                (jnp.int32(0), jnp.int32(0), jnp.zeros((n_tok + chunk, width), tab_loc.dtype)),
            )
            tgt_rows, my_cand_rows = got[:n_tok], got[n_tok:]
            cand_rows = lax.all_gather(my_cand_rows, ALL_AXES, tiled=True)

            z_tgt = jnp.einsum("td,td->t", hidden, tgt_rows, preferred_element_type=jnp.float32)
            z_cand = jnp.einsum("td,sd->ts", hidden, cand_rows, preferred_element_type=jnp.float32) - log_q[None, :]
            z_cand = jnp.where(y_loc[:, None] == cand_ids[None, :], -1e9, z_cand)
            row_max = jnp.maximum(z_tgt, jnp.max(z_cand, axis=1))
            e_tgt = jnp.exp(z_tgt - row_max)
            e_cand = jnp.exp(z_cand - row_max[:, None])
            exp_total = e_tgt + jnp.sum(e_cand, axis=1)
            loss_sum = jnp.sum(row_max + jnp.log(exp_total) - z_tgt)

            dz_tgt = (e_tgt / exp_total - 1.0) / n_total
            dz_cand = (e_cand / exp_total[:, None] / n_total).astype(jnp.bfloat16)
            grad_hid = (dz_tgt[:, None] * tgt_rows + jnp.dot(dz_cand, cand_rows, preferred_element_type=jnp.float32)).astype(jnp.bfloat16)
            cand_grad = jnp.einsum("ts,td->sd", dz_cand, hidden, preferred_element_type=jnp.float32)
            grad_down = jnp.einsum("tf,td->fd", act_b, grad_hid, preferred_element_type=jnp.float32)
            grad_act = jnp.einsum("td,fd->tf", grad_hid, w_down, preferred_element_type=jnp.float32)
            grad_pre = gelu_vjp(grad_act)[0].astype(jnp.bfloat16)
            grad_up = jnp.einsum("ti,tf->if", x_loc, grad_pre, preferred_element_type=jnp.float32)
            cand_grad, grad_up, grad_down = lax.psum((cand_grad, grad_up, grad_down), ALL_AXES)

            t_rank, t_owner, t_local = rank[:n_tok], owner[:n_tok], local[:n_tok]
            t_count = jnp.sum((t_owner[:, None] == jnp.arange(n_row)[None, :]).astype(jnp.int32), axis=0)
            c_rank, _ = ranks(owner[n_tok:], n_row)
            c_slot = owner[n_tok:] * chunk + c_rank
            c_count = per_owner - t_count
            c_row, c_pos = to_slots(c_slot, [(local[n_tok:] - rows_local).astype(jnp.float32), jnp.arange(chunk, dtype=jnp.float32)], n_row * chunk)
            c_row = (c_row + rows_local).reshape(n_row, chunk)
            c_pos = c_pos.reshape(n_row, chunk)

            def give_round(carry):
                k, grad = carry
                slot = slots_of(k, t_rank, t_owner)
                t_row, t_pos, t_dz = to_slots(
                    slot, [(t_local - rows_local).astype(jnp.float32), jnp.arange(n_tok), dz_tgt], n_slots)
                t_row = t_row + rows_local
                now = jnp.clip(t_count - k * CAP, 0, CAP).astype(jnp.float32)
                counts = jnp.stack([now, c_count.astype(jnp.float32), jnp.full((n_row,), loss_sum)], axis=1)
                hid_out = jnp.take(hidden, t_pos, axis=0, mode="clip").reshape(n_row, CAP, width)
                meta = tile_rows([t_row.reshape(n_row, CAP), t_dz.reshape(n_row, CAP), c_row, c_pos, counts], n_row)
                hid_in, meta_in = exchange(n_row, n_dp, True, hid_out, meta)
                vals = meta_in[:, 1, :CAP, None] * hid_in.astype(jnp.float32)
                row_ids = meta_in[:, 0, :CAP].astype(jnp.int32)
                grad = add_rows(grad, vals.reshape(n_dev * CAP, width), row_ids, meta_in[:, 4, 0].astype(jnp.int32))
                return k + 1, grad, meta_in[:, 2, :chunk].astype(jnp.int32), meta_in[:, 3, :chunk].astype(jnp.int32), meta_in[:, 4, 1].astype(jnp.int32), jnp.sum(meta_in[:, 4, 2])

            grad0 = jnp.zeros((rows_local + 8, width), jnp.float32)
            k, grad, c_rows_in, c_pos_in, c_n, loss_all = give_round((jnp.int32(0), grad0))
            _, grad = lax.while_loop(
                lambda c: c[0] * CAP < most_all, lambda c: give_round(c)[:2], (k, grad))
            c_vals = jnp.take(cand_grad, (c_pos_in + chunk * jnp.arange(n_dev)[:, None]).reshape(-1), axis=0, mode="clip")
            grad = add_rows(grad, c_vals, c_rows_in, c_n)
            return loss_all / n_total, grad[:rows_local], grad_up, grad_down

        return jax.shard_map(
            device_step,
            mesh=mesh,
            in_specs=(P(ALL_AXES, None), P(), P(), P("row", None), P(), P(), P(ALL_AXES)),
            out_specs=(P(), P("row", None), P(), P()),
            check_vma=False,
        )(x_tok, w_up, w_down, item_table, cand_ids, log_q, targets)

    return run_step
```

```python
import functools

import jax
import jax.numpy as jnp
from jax import lax
from jax.experimental import pallas as pl
from jax.experimental.pallas import tpu as pltpu
from jax.sharding import PartitionSpec as P

ALL_AXES = ("dp", "row")
MESH = pl.DeviceIdType.MESH
CAP = 96
BLK = 512
TOK = 256
LANES = 128
ANY = pl.BlockSpec(memory_space=pl.ANY)
VMEM = pl.BlockSpec(memory_space=pltpu.VMEM)
SMEM = pl.BlockSpec(memory_space=pltpu.SMEM)


def params():
    return pltpu.CompilerParams(has_side_effects=True, vmem_limit_bytes=60 * 1024 * 1024)


def exchange(n_row, n_dp, both, *xs):
    n_x = len(xs)
    steps = range(n_dp) if both else range(1)
    n_out = n_row * (n_dp if both else 1)

    def kernel(*refs):
        ins, outs = refs[:n_x], refs[n_x:2 * n_x]
        send_sem, recv_sem = refs[2 * n_x:]
        row, dp = lax.axis_index("row"), lax.axis_index("dp")
        slot = dp * n_row + row if both else row
        for i in range(n_x):
            pltpu.make_async_copy(ins[i].at[row], outs[i].at[slot], recv_sem.at[i]).start()

        for e in steps:
            def send(j, carry, e=e):
                peer = lax.rem(row + j, n_row)
                for i in range(n_x):
                    pltpu.make_async_remote_copy(
                        src_ref=ins[i].at[peer],
                        dst_ref=outs[i].at[slot],
                        send_sem=send_sem.at[i, e],
                        recv_sem=recv_sem.at[i],
                        device_id={"row": peer, "dp": lax.rem(dp + e, n_dp)},
                        device_id_type=MESH,
                    ).start()
                return carry
            lax.fori_loop(0 if e else 1, n_row, send, 0)
        for i in range(n_x):
            for e in steps:
                sent = ins[i] if e else ins[i].at[pl.ds(0, n_row - 1)]
                pltpu.make_async_copy(sent, sent, send_sem.at[i, e]).wait()
            pltpu.make_async_copy(outs[i], outs[i], recv_sem.at[i]).wait()

    return pl.pallas_call(
        kernel,
        out_shape=[jax.ShapeDtypeStruct((n_out,) + x.shape[1:], x.dtype) for x in xs],
        in_specs=[VMEM] * n_x,
        out_specs=[VMEM] * n_x,
        scratch_shapes=[pltpu.SemaphoreType.DMA((n_x, n_dp)), pltpu.SemaphoreType.DMA((n_x,))],
        compiler_params=params(),
    )(*xs)


def pack(slot_row, vals, n_row):
    n_pad = slot_row.shape[1]
    per = 4 if n_row % 4 == 0 else 1

    def kernel(slot_ref, vals_ref, hid_ref, want_ref):
        base = pl.program_id(0) * (per * LANES)
        at = lax.broadcasted_iota(jnp.int32, (per * LANES, n_pad), 0) + base
        hit = (at == slot_ref[...]).astype(jnp.float32).astype(jnp.bfloat16)
        got = jnp.dot(hit, vals_ref[...], preferred_element_type=jnp.float32)
        for o in range(per):
            blk = got[o * LANES:(o + 1) * LANES]
            hid_ref[o] = blk[:CAP, :LANES].astype(jnp.bfloat16)
            ids = jnp.transpose(blk[:, LANES:])
            want_ref[o] = (ids[0:1] * 128.0 + ids[1:2]).astype(jnp.int32)

    return pl.pallas_call(
        kernel,
        grid=(n_row // per,),
        out_shape=[
            jax.ShapeDtypeStruct((n_row, CAP, LANES), jnp.bfloat16),
            jax.ShapeDtypeStruct((n_row, 1, LANES), jnp.int32),
        ],
        in_specs=[pl.BlockSpec((1, n_pad), lambda i: (0, 0)), pl.BlockSpec((n_pad, 2 * LANES), lambda i: (0, 0))],
        out_specs=[
            pl.BlockSpec((per, CAP, LANES), lambda i: (i, 0, 0)),
            pl.BlockSpec((per, 1, LANES), lambda i: (i, 0, 0)),
        ],
        compiler_params=pltpu.CompilerParams(vmem_limit_bytes=40 * 1024 * 1024),
    )(slot_row, vals)


def fetch(n_row, n_dp, want, table):
    rows_local, width = table.shape
    cut = min(1024, rows_local // 2)
    n_cut = rows_local // cut

    def kernel(want_ref, tab_ref, rows_ref, most_ref, tab16, tab32, asked, ask_s, stage, out_buf, sems, tab_sem):
        row, dp = lax.axis_index("row"), lax.axis_index("dp")

        def load(k, p):
            sl = pl.ds(pl.multiple_of(k * cut, cut), cut)
            return pltpu.make_async_copy(tab_ref.at[sl], tab16.at[p], tab_sem.at[p])
        load(0, 0).start()
        load(1, 1).start()
        pltpu.make_async_copy(want_ref.at[row], asked.at[row], sems.at[1]).start()

        def ask(j, carry):
            peer = lax.rem(row + j, n_row)
            pltpu.make_async_remote_copy(
                src_ref=want_ref.at[peer], dst_ref=asked.at[row], send_sem=sems.at[0], recv_sem=sems.at[1],
                device_id={"row": peer, "dp": dp}, device_id_type=MESH).start()
            return carry
        lax.fori_loop(1, n_row, ask, 0)

        def widen(k, more):
            for p in range(2):
                load(2 * k + p, p).wait()
                sl = pl.ds(pl.multiple_of((2 * k + p) * cut, cut), cut)
                tab32[sl, :] = tab16[p].astype(jnp.float32)
                if more:
                    load(2 * k + p + 2, p).start()
            return 0
        lax.fori_loop(0, n_cut // 2 - 1, lambda k, c: widen(k, True), 0)
        widen(n_cut // 2 - 1, False)
        pltpu.make_async_copy(asked, asked, sems.at[1]).wait()
        to_s = pltpu.make_async_copy(asked, ask_s, tab_sem.at[0])
        to_s.start()
        most_ref[...] = jnp.broadcast_to(jnp.max(asked[...], axis=0), (8, LANES))
        to_s.wait()

        def send(peer):
            pltpu.make_async_remote_copy(
                src_ref=out_buf.at[peer], dst_ref=rows_ref.at[row], send_sem=sems.at[2], recv_sem=sems.at[3],
                device_id={"row": peer, "dp": dp}, device_id_type=MESH).start()

        def gather(j):
            peer = lax.rem(row + j, n_row)
            for c in range(CAP):
                stage[pl.ds(c, 1), :] = tab32[pl.ds(ask_s[peer, 0, c], 1), :]
            out_buf[peer] = stage[...].astype(jnp.bfloat16)

        gather(1)

        def step(j, carry):
            gather(j)
            send(lax.rem(row + j - 1, n_row))
            return carry
        lax.fori_loop(2, n_row, step, 0)
        gather(n_row)
        send(lax.rem(row + n_row - 1, n_row))
        pltpu.make_async_copy(out_buf.at[row], rows_ref.at[row], sems.at[3]).start()
        sent = want_ref.at[pl.ds(0, n_row - 1)]
        pltpu.make_async_copy(sent, sent, sems.at[0]).wait()
        sent = out_buf.at[pl.ds(0, n_row - 1)]
        pltpu.make_async_copy(sent, sent, sems.at[2]).wait()
        pltpu.make_async_copy(rows_ref, rows_ref, sems.at[3]).wait()

    return pl.pallas_call(
        kernel,
        out_shape=[
            jax.ShapeDtypeStruct((n_row, CAP, width), table.dtype),
            jax.ShapeDtypeStruct((8, LANES), jnp.int32),
        ],
        in_specs=[VMEM, ANY],
        out_specs=[VMEM, VMEM],
        scratch_shapes=[
            pltpu.VMEM((2, cut, width), table.dtype),
            pltpu.VMEM((rows_local, width), jnp.float32),
            pltpu.VMEM((n_row, 1, LANES), jnp.int32),
            pltpu.SMEM((n_row, 1, LANES), jnp.int32),
            pltpu.VMEM((CAP, width), jnp.float32),
            pltpu.VMEM((n_row, CAP, width), table.dtype),
            pltpu.SemaphoreType.DMA((4,)),
            pltpu.SemaphoreType.DMA((2,)),
        ],
        compiler_params=params(),
    )(want, table)


def gather_cands(n_row, n_dp, my_cands, most):
    chunk, width = my_cands.shape

    def kernel(mine_ref, most_ref, all_ref, top_ref, theirs, sems):
        row, dp = lax.axis_index("row"), lax.axis_index("dp")
        other = lax.rem(dp + 1, n_dp)
        me = dp * n_row + row

        def one(j, carry):
            peer = lax.rem(row + j, n_row)
            pltpu.make_async_remote_copy(
                src_ref=mine_ref, dst_ref=all_ref.at[me], send_sem=sems.at[0], recv_sem=sems.at[1],
                device_id={"row": peer, "dp": dp}, device_id_type=MESH).start()
            return carry
        lax.fori_loop(1, n_row, one, 0)
        pltpu.make_async_copy(mine_ref, all_ref.at[me], sems.at[1]).start()
        count = pltpu.make_async_remote_copy(
            src_ref=most_ref, dst_ref=theirs, send_sem=sems.at[4], recv_sem=sems.at[5],
            device_id={"row": row, "dp": other}, device_id_type=MESH)
        count.start()
        half = all_ref.at[pl.ds(dp * n_row, n_row)]
        pltpu.make_async_copy(half, half, sems.at[1]).wait()
        swap = pltpu.make_async_remote_copy(
            src_ref=half, dst_ref=half, send_sem=sems.at[2], recv_sem=sems.at[3],
            device_id={"row": row, "dp": other}, device_id_type=MESH)
        swap.start()
        count.wait()
        top_ref[...] = jnp.maximum(most_ref[...], theirs[...])
        sent = all_ref.at[pl.ds(0, n_row - 1)]
        pltpu.make_async_copy(sent, sent, sems.at[0]).wait()
        swap.wait()

    return pl.pallas_call(
        kernel,
        out_shape=[
            jax.ShapeDtypeStruct((n_dp * n_row, chunk, width), my_cands.dtype),
            jax.ShapeDtypeStruct(most.shape, most.dtype),
        ],
        in_specs=[VMEM, VMEM],
        out_specs=[VMEM, VMEM],
        scratch_shapes=[pltpu.VMEM(most.shape, most.dtype), pltpu.SemaphoreType.DMA((6,))],
        compiler_params=params(),
    )(my_cands, most)


def softmax(n_total, cand_rows, hidden, tgt, y_lanes, cand_ids, log_q):
    n_cand, width = cand_rows.shape
    n_tok = hidden.shape[0]
    n_blk, n_sub = n_cand // BLK, n_tok // TOK
    f32 = jnp.float32

    def kernel(cands, h_ref, t_ref, y_ref, id_ref, lq_ref, cg_ref, dh_ref, dz_ref, loss_ref, z, g, h_t, acc, stat):
        h_t[...] = jnp.transpose(h_ref[...].astype(f32)).astype(jnp.bfloat16)
        for s in range(n_sub):
            tok = pl.ds(s * TOK, TOK)
            prod = h_ref[tok, :].astype(f32) * t_ref[tok, :].astype(f32)
            z_tgt = jnp.broadcast_to(jnp.sum(prod, axis=1, keepdims=True), (TOK, LANES))
            stat[0, tok, :] = z_tgt
            stat[1, tok, :] = z_tgt
        def logits(b, carry):
            rows = cands[pl.ds(pl.multiple_of(b * BLK, BLK), BLK), :]
            cols = pl.ds(pl.multiple_of(b * BLK, BLK), BLK)
            lq, cid = lq_ref[:, cols], id_ref[:, cols]

            def sub(s, c2):
                tok = pl.ds(pl.multiple_of(s * TOK, TOK), TOK)
                zz = lax.dot_general(h_ref[tok, :], rows, (((1,), (1,)), ((), ())), preferred_element_type=f32) - lq
                y = y_ref[tok, :]
                top = stat[1, tok, :]
                for k in range(BLK // LANES):
                    ln = slice(k * LANES, (k + 1) * LANES)
                    part = jnp.where(y == cid[:, ln], -1e9, zz[:, ln])
                    z[tok, pl.ds(pl.multiple_of(b * BLK + k * LANES, LANES), LANES)] = part
                    top = jnp.maximum(top, part)
                stat[1, tok, :] = top
                return c2
            return lax.fori_loop(0, n_sub, sub, carry)
        lax.fori_loop(0, n_blk, logits, 0)

        for s in range(n_sub):
            tok = pl.ds(s * TOK, TOK)
            stat[1, tok, :] = jnp.broadcast_to(jnp.max(stat[1, tok, :], axis=1, keepdims=True), (TOK, LANES))
            stat[2, tok, :] = jnp.zeros((TOK, LANES), f32)

        def exps(b, carry):
            def sub(s, c2):
                tok = pl.ds(pl.multiple_of(s * TOK, TOK), TOK)
                top = stat[1, tok, :]
                tot = stat[2, tok, :]
                for k in range(BLK // LANES):
                    at = pl.ds(pl.multiple_of(b * BLK + k * LANES, LANES), LANES)
                    e = jnp.exp(z[tok, at] - top)
                    z[tok, at] = e
                    tot = tot + e
                stat[2, tok, :] = tot
                return c2
            return lax.fori_loop(0, n_sub, sub, carry)
        lax.fori_loop(0, n_blk, exps, 0)

        loss_ref[...] = jnp.zeros_like(loss_ref)
        for s in range(n_sub):
            tok = pl.ds(s * TOK, TOK)
            z_tgt, top = stat[0, tok, :], stat[1, tok, :]
            e_tgt = jnp.exp(z_tgt - top)
            total = e_tgt + jnp.broadcast_to(jnp.sum(stat[2, tok, :], axis=1, keepdims=True), (TOK, LANES))
            dz = (e_tgt / total - 1.0) * (1.0 / n_total)
            dz_ref[tok, :] = dz
            stat[2, tok, :] = (1.0 / total) * (1.0 / n_total)
            part = top + jnp.log(total) - z_tgt
            loss_ref[...] += jnp.broadcast_to(jnp.sum(part, axis=0, keepdims=True), loss_ref.shape)
            acc[tok, :] = dz * t_ref[tok, :].astype(f32)

        def grads(b, carry):
            rows = cands[pl.ds(pl.multiple_of(b * BLK, BLK), BLK), :]

            def sub(s, c2):
                tok = pl.ds(pl.multiple_of(s * TOK, TOK), TOK)
                inv = stat[2, tok, :]
                for k in range(BLK // LANES):
                    at = pl.ds(pl.multiple_of(b * BLK + k * LANES, LANES), LANES)
                    g[tok, k * LANES:(k + 1) * LANES] = (z[tok, at] * inv).astype(jnp.bfloat16)
                acc[tok, :] += jnp.dot(g[tok, :], rows, preferred_element_type=f32)
                return c2
            lax.fori_loop(0, n_sub, sub, 0)
            cg_t = jnp.dot(h_t[...], g[...], preferred_element_type=f32)
            cg_ref[pl.ds(pl.multiple_of(b * BLK, BLK), BLK), :] = jnp.transpose(cg_t)
            return carry
        lax.fori_loop(0, n_blk, grads, 0)
        dh_ref[...] = acc[...].astype(jnp.bfloat16)

    return pl.pallas_call(
        kernel,
        out_shape=[
            jax.ShapeDtypeStruct((n_cand, width), f32),
            jax.ShapeDtypeStruct((n_tok, width), jnp.bfloat16),
            jax.ShapeDtypeStruct((n_tok, LANES), f32),
            jax.ShapeDtypeStruct((8, LANES), f32),
        ],
        in_specs=[VMEM] * 6,
        out_specs=[VMEM] * 4,
        scratch_shapes=[
            pltpu.VMEM((n_tok, n_cand), f32),
            pltpu.VMEM((n_tok, BLK), jnp.bfloat16),
            pltpu.VMEM((width, n_tok), jnp.bfloat16),
            pltpu.VMEM((n_tok, width), f32),
            pltpu.VMEM((3, n_tok, LANES), f32),
        ],
        compiler_params=pltpu.CompilerParams(vmem_limit_bytes=60 * 1024 * 1024),
    )(cand_rows, hidden, tgt, y_lanes, cand_ids, log_q)


def add_rows(grad, vals, row_ids, counts, val_ids=None, n_rows=None, n_acc=2):
    n_list, width = row_ids.shape[0], vals.shape[1]
    per_list = vals.shape[0] // n_list
    n_full = n_rows + 8 if grad is None else grad.shape[0]
    n_out = n_full if n_rows is None or grad is None else n_rows
    chunk = 512

    def kernel(*refs):
        idx, cnt, vals_ref = refs[:3]
        rest = list(refs[3:])
        vid = rest.pop(0) if val_ids is not None else None
        grad_ref = rest.pop(0) if grad is not None else None
        out_ref, sem = rest[0], rest[-1]
        accs = rest[1:-1]
        if grad_ref is not None:
            cp_in = pltpu.make_async_copy(grad_ref, accs[0], sem)
            cp_in.start()
        fresh = accs if grad_ref is None else accs[1:]

        def clear(k, carry):
            for a in fresh:
                a[pl.ds(pl.multiple_of(k * 8, 8), 8), :] = jnp.zeros((8, width), jnp.float32)
            return carry
        if fresh:
            lax.fori_loop(0, n_full // 8, clear, 0, unroll=False)
        if grad_ref is not None:
            cp_in.wait()

        def one_list(i, carry):
            def group(q, c2):
                for u in range(8):
                    c = q * 8 + u
                    acc = accs[u % n_acc]
                    r = idx[i, c]
                    v = i * per_list + c if vid is None else vid[i, c]
                    acc[pl.ds(r, 1), :] += vals_ref[pl.ds(v, 1), :]
                return c2
            return lax.fori_loop(0, (cnt[i] + 7) // 8, group, carry)
        lax.fori_loop(0, n_list, one_list, 0)

        if n_acc > 1:
            def merge(k, carry):
                sl = pl.ds(pl.multiple_of(k * 8, 8), 8)
                tot = accs[0][sl, :]
                for a in accs[1:]:
                    tot = tot + a[sl, :]
                accs[0][sl, :] = tot
                return carry
            lax.fori_loop(0, n_full // 8, merge, 0)
        cp_out = pltpu.make_async_copy(accs[0].at[pl.ds(0, n_out)], out_ref, sem)
        cp_out.start()
        cp_out.wait()

    args = [row_ids, counts, vals]
    specs = [SMEM, SMEM, VMEM]
    if val_ids is not None:
        args.append(val_ids)
        specs.append(SMEM)
    if grad is not None:
        args.append(grad)
        specs.append(ANY)
    return pl.pallas_call(
        kernel,
        out_shape=jax.ShapeDtypeStruct((n_out, width), jnp.float32),
        in_specs=specs,
        out_specs=ANY,
        scratch_shapes=[pltpu.VMEM((n_full, width), jnp.float32)] * n_acc + [pltpu.SemaphoreType.DMA],
        compiler_params=pltpu.CompilerParams(vmem_limit_bytes=60 * 1024 * 1024),
    )(*args)


def ranks(owner, n_row):
    n = owner.shape[0]
    hot = (owner[:, None] == jnp.arange(n_row)[None, :]).astype(jnp.bfloat16)
    pos = jnp.arange(n)
    before = (pos[:, None] > pos[None, :]).astype(jnp.bfloat16)
    earlier = jnp.dot(before, hot, preferred_element_type=jnp.float32)
    hot32 = hot.astype(jnp.float32)
    return jnp.sum(earlier * hot32, axis=1).astype(jnp.int32), jnp.sum(hot32, axis=0).astype(jnp.int32)


def to_slots(slot, vals, n_slots):
    hit = slot[:, None] == jnp.arange(n_slots)[None, :]
    return [jnp.sum(jnp.where(hit, v[:, None], jnp.zeros((), v.dtype)), axis=0) for v in vals]


def tile_rows(rows, n_row):
    padded = [jnp.pad(r, ((0, 0), (0, LANES - r.shape[1]))) for r in rows]
    padded += [jnp.zeros_like(padded[0])] * (8 - len(rows))
    return jnp.stack(padded, axis=1)


def solution(mesh):
    n_row, n_dp = mesh.shape["row"], mesh.shape["dp"]
    n_dev = n_row * n_dp

    def run_step(x_tok, w_up, w_down, item_table, cand_ids, log_q, targets):
        n_total = x_tok.shape[0]

        def device_step(x_loc, w_up, w_down, tab_loc, cand_ids, log_q, y_loc):
            rows_local, width = tab_loc.shape
            n_tok = y_loc.shape[0]
            n_cand = cand_ids.shape[0]
            row, dp = lax.axis_index("row"), lax.axis_index("dp")
            me = dp * n_row + row
            chunk = n_cand // n_dev
            f32, bf16 = jnp.float32, jnp.bfloat16
            n_ids = n_tok + chunk
            n_pad = -(-n_ids // LANES) * LANES

            my_cands = lax.dynamic_slice_in_dim(cand_ids, me * chunk, chunk)
            ids = jnp.concatenate([y_loc, my_cands])
            owner, local = ids // rows_local, ids % rows_local
            rank, per_owner = ranks(owner, n_row)
            most = jnp.max(per_owner)

            pre_act = jnp.dot(x_loc, w_up, preferred_element_type=f32)
            act_full, gelu_vjp = jax.vjp(jax.nn.gelu, pre_act)
            act_b = act_full.astype(bf16)
            hidden = jnp.dot(act_b, w_down, preferred_element_type=f32).astype(bf16)

            split = jnp.pad(jnp.stack([local // 128, local % 128], axis=1).astype(bf16), ((0, n_pad - n_ids), (0, LANES - 2)))
            carried = jnp.concatenate([jnp.pad(hidden, ((0, n_pad - n_tok), (0, 0))), split], axis=1)

            def pack_round(k):
                rel = rank - k * CAP
                hit = (rel >= 0) & (rel < CAP)
                slot = jnp.where(hit, owner * LANES + rel, -1)
                hid_out, want = pack(jnp.pad(slot, (0, n_pad - n_ids), constant_values=-1)[None, :], carried, n_row)
                return hit, owner * CAP + rel, hid_out, want

            def fetch_round(k):
                hit, at, hid_out, want = pack_round(k)
                lane = jnp.arange(LANES)[None, None, :]
                rows_in, most_all = fetch(n_row, n_dp, jnp.where(lane == LANES - 1, most, want), tab_loc)
                got = jnp.take(rows_in.reshape(n_row * CAP, width), at, axis=0, mode="clip")
                return hit, got, hid_out, most_all

            _, got, hid_out, most_dp = fetch_round(0)
            cand_rows, most_all = gather_cands(n_row, n_dp, got[n_tok:], most_dp)
            most_all = most_all[0, LANES - 1]

            def fetch_more(carry):
                k, got, _ = carry
                hit, new, _, most = fetch_round(k)
                got = jnp.where(hit[:, None], new, got)
                return k + 1, got, gather_cands(n_row, n_dp, got[n_tok:], most)[0]

            _, got, cand_rows = lax.while_loop(
                lambda c: c[0] * CAP < most_all, fetch_more, (jnp.int32(1), got, cand_rows))
            tgt_rows, cand_rows = got[:n_tok], cand_rows.reshape(n_cand, width)

            cand_grad, grad_hid, dz_lanes, loss_part = softmax(
                n_total, cand_rows, hidden, tgt_rows,
                jnp.broadcast_to(y_loc[:, None], (n_tok, LANES)), cand_ids[None, :], log_q[None, :])
            dz_tgt, loss_sum = dz_lanes[:, 0], loss_part[0, 0]

            grad_down = jnp.einsum("tf,td->fd", act_b, grad_hid, preferred_element_type=f32)
            grad_act = jnp.einsum("td,fd->tf", grad_hid, w_down, preferred_element_type=f32)
            grad_pre = gelu_vjp(grad_act)[0].astype(bf16)
            grad_up = jnp.einsum("ti,tf->if", x_loc, grad_pre, preferred_element_type=f32)
            cand_grad, grad_up, grad_down = lax.psum((cand_grad, grad_up, grad_down), ALL_AXES)

            t_rank, t_owner, t_local = rank[:n_tok], owner[:n_tok], local[:n_tok]
            t_count = jnp.sum((t_owner[:, None] == jnp.arange(n_row)[None, :]).astype(jnp.int32), axis=0)
            c_rank, _ = ranks(owner[n_tok:], n_row)
            c_slot = owner[n_tok:] * chunk + c_rank
            c_count = per_owner - t_count
            c_row, c_pos = to_slots(c_slot, [(local[n_tok:] - rows_local).astype(f32), jnp.arange(chunk, dtype=f32)], n_row * chunk)
            c_row = (c_row + rows_local).reshape(n_row, chunk)
            c_pos = c_pos.reshape(n_row, chunk) + (me * chunk).astype(f32)

            def give_round(k, grad, hid_out):
                rel = t_rank - k * CAP
                slot = jnp.where((rel >= 0) & (rel < CAP), t_owner * CAP + rel, -1)
                t_row, t_dz = to_slots(slot, [t_local.astype(f32), dz_tgt], n_row * CAP)
                now = jnp.clip(t_count - k * CAP, 0, CAP).astype(f32)
                counts = jnp.stack([now, c_count.astype(f32), jnp.full((n_row,), loss_sum)], axis=1)
                meta = tile_rows([t_row.reshape(n_row, CAP), t_dz.reshape(n_row, CAP), c_row, c_pos, counts], n_row)
                hid_in, meta_in = exchange(n_row, n_dp, True, hid_out, meta)
                vals = meta_in[:, 1, :CAP, None] * hid_in.astype(f32)
                grad = add_rows(grad, vals.reshape(n_dev * CAP, width), meta_in[:, 0, :CAP].astype(jnp.int32),
                                meta_in[:, 4, 0].astype(jnp.int32), n_rows=rows_local if grad is None else None)
                return grad, meta_in

            grad, meta_in = give_round(0, None, hid_out)
            _, grad = lax.while_loop(
                lambda c: c[0] * CAP < most_all,
                lambda c: (c[0] + 1, give_round(c[0], c[1], pack_round(c[0])[2])[0]), (jnp.int32(1), grad))
            to_int = lambda v: v.astype(jnp.int32)
            grad = add_rows(grad, cand_grad, to_int(meta_in[:, 2, :chunk]), to_int(meta_in[:, 4, 1]),
                            val_ids=to_int(meta_in[:, 3, :chunk]), n_rows=rows_local, n_acc=1)
            return jnp.sum(meta_in[:, 4, 2]) / n_total, grad, grad_up, grad_down

        return jax.shard_map(
            device_step,
            mesh=mesh,
            in_specs=(P(ALL_AXES, None), P(), P(), P("row", None), P(), P(), P(ALL_AXES)),
            out_specs=(P(), P("row", None), P(), P()),
            check_vma=False,
        )(x_tok, w_up, w_down, item_table, cand_ids, log_q, targets)

    return run_step
```

```python
import functools

import jax
import jax.numpy as jnp
from jax import lax
from jax.experimental import pallas as pl
from jax.experimental.pallas import tpu as pltpu
from jax.sharding import PartitionSpec as P

ALL_AXES = ("dp", "row")
MESH = pl.DeviceIdType.MESH
CAP = 96
BLK = 512
TOK = 256
LANES = 128
ANY = pl.BlockSpec(memory_space=pl.ANY)
VMEM = pl.BlockSpec(memory_space=pltpu.VMEM)
SMEM = pl.BlockSpec(memory_space=pltpu.SMEM)


def params():
    return pltpu.CompilerParams(has_side_effects=True, vmem_limit_bytes=60 * 1024 * 1024)


def exchange(n_row, n_dp, both, *xs):
    n_x = len(xs)
    steps = range(n_dp) if both else range(1)
    n_out = n_row * (n_dp if both else 1)

    def kernel(*refs):
        ins, outs = refs[:n_x], refs[n_x:2 * n_x]
        send_sem, recv_sem = refs[2 * n_x:]
        row, dp = lax.axis_index("row"), lax.axis_index("dp")
        slot = dp * n_row + row if both else row
        for i in range(n_x):
            pltpu.make_async_copy(ins[i].at[row], outs[i].at[slot], recv_sem.at[i]).start()

        for e in steps:
            def send(j, carry, e=e):
                peer = lax.rem(row + j, n_row)
                for i in range(n_x):
                    pltpu.make_async_remote_copy(
                        src_ref=ins[i].at[peer],
                        dst_ref=outs[i].at[slot],
                        send_sem=send_sem.at[i, e],
                        recv_sem=recv_sem.at[i],
                        device_id={"row": peer, "dp": lax.rem(dp + e, n_dp)},
                        device_id_type=MESH,
                    ).start()
                return carry
            lax.fori_loop(0 if e else 1, n_row, send, 0)
        for i in range(n_x):
            for e in steps:
                sent = ins[i] if e else ins[i].at[pl.ds(0, n_row - 1)]
                pltpu.make_async_copy(sent, sent, send_sem.at[i, e]).wait()
            pltpu.make_async_copy(outs[i], outs[i], recv_sem.at[i]).wait()

    return pl.pallas_call(
        kernel,
        out_shape=[jax.ShapeDtypeStruct((n_out,) + x.shape[1:], x.dtype) for x in xs],
        in_specs=[VMEM] * n_x,
        out_specs=[VMEM] * n_x,
        scratch_shapes=[pltpu.SemaphoreType.DMA((n_x, n_dp)), pltpu.SemaphoreType.DMA((n_x,))],
        compiler_params=params(),
    )(*xs)


def pack(slot_row, vals, n_row):
    n_pad = slot_row.shape[1]
    per = 4 if n_row % 4 == 0 else 1

    def kernel(slot_ref, vals_ref, hid_ref, want_ref):
        base = pl.program_id(0) * (per * LANES)
        at = lax.broadcasted_iota(jnp.int32, (per * LANES, n_pad), 0) + base
        hit = (at == slot_ref[...]).astype(jnp.float32).astype(jnp.bfloat16)
        got = jnp.dot(hit, vals_ref[...], preferred_element_type=jnp.float32)
        for o in range(per):
            blk = got[o * LANES:(o + 1) * LANES]
            hid_ref[o] = blk[:CAP, :LANES].astype(jnp.bfloat16)
            ids = jnp.transpose(blk[:, LANES:])
            want_ref[o] = (ids[0:1] * 128.0 + ids[1:2]).astype(jnp.int32)

    return pl.pallas_call(
        kernel,
        grid=(n_row // per,),
        out_shape=[
            jax.ShapeDtypeStruct((n_row, CAP, LANES), jnp.bfloat16),
            jax.ShapeDtypeStruct((n_row, 1, LANES), jnp.int32),
        ],
        in_specs=[pl.BlockSpec((1, n_pad), lambda i: (0, 0)), pl.BlockSpec((n_pad, 2 * LANES), lambda i: (0, 0))],
        out_specs=[
            pl.BlockSpec((per, CAP, LANES), lambda i: (i, 0, 0)),
            pl.BlockSpec((per, 1, LANES), lambda i: (i, 0, 0)),
        ],
        compiler_params=pltpu.CompilerParams(vmem_limit_bytes=40 * 1024 * 1024),
    )(slot_row, vals)


def fetch(n_row, n_dp, want, table):
    rows_local, width = table.shape
    cut = min(1024, rows_local // 2)
    n_cut = rows_local // cut

    def kernel(want_ref, tab_ref, rows_ref, most_ref, tab16, tab32, asked, ask_s, stage, out_buf, sems, tab_sem):
        row, dp = lax.axis_index("row"), lax.axis_index("dp")

        def load(k, p):
            sl = pl.ds(pl.multiple_of(k * cut, cut), cut)
            return pltpu.make_async_copy(tab_ref.at[sl], tab16.at[p], tab_sem.at[p])
        load(0, 0).start()
        load(1, 1).start()
        pltpu.make_async_copy(want_ref.at[row], asked.at[row], sems.at[1]).start()

        def ask(j, carry):
            peer = lax.rem(row + j, n_row)
            pltpu.make_async_remote_copy(
                src_ref=want_ref.at[peer], dst_ref=asked.at[row], send_sem=sems.at[0], recv_sem=sems.at[1],
                device_id={"row": peer, "dp": dp}, device_id_type=MESH).start()
            return carry
        lax.fori_loop(1, n_row, ask, 0)

        def widen(k, more):
            for p in range(2):
                load(2 * k + p, p).wait()
                sl = pl.ds(pl.multiple_of((2 * k + p) * cut, cut), cut)
                tab32[sl, :] = tab16[p].astype(jnp.float32)
                if more:
                    load(2 * k + p + 2, p).start()
            return 0
        lax.fori_loop(0, n_cut // 2 - 1, lambda k, c: widen(k, True), 0)
        widen(n_cut // 2 - 1, False)
        pltpu.make_async_copy(asked, asked, sems.at[1]).wait()
        to_s = pltpu.make_async_copy(asked, ask_s, tab_sem.at[0])
        to_s.start()
        most_ref[...] = jnp.broadcast_to(jnp.max(asked[...], axis=0), (8, LANES))
        to_s.wait()

        def send(peer):
            pltpu.make_async_remote_copy(
                src_ref=out_buf.at[peer], dst_ref=rows_ref.at[row], send_sem=sems.at[2], recv_sem=sems.at[3],
                device_id={"row": peer, "dp": dp}, device_id_type=MESH).start()

        def gather(j):
            peer = lax.rem(row + j, n_row)
            for c in range(CAP):
                stage[pl.ds(c, 1), :] = tab32[pl.ds(ask_s[peer, 0, c], 1), :]
            out_buf[peer] = stage[...].astype(jnp.bfloat16)

        gather(1)

        def step(j, carry):
            gather(j)
            send(lax.rem(row + j - 1, n_row))
            return carry
        lax.fori_loop(2, n_row, step, 0)
        gather(n_row)
        send(lax.rem(row + n_row - 1, n_row))
        pltpu.make_async_copy(out_buf.at[row], rows_ref.at[row], sems.at[3]).start()
        sent = want_ref.at[pl.ds(0, n_row - 1)]
        pltpu.make_async_copy(sent, sent, sems.at[0]).wait()
        sent = out_buf.at[pl.ds(0, n_row - 1)]
        pltpu.make_async_copy(sent, sent, sems.at[2]).wait()
        pltpu.make_async_copy(rows_ref, rows_ref, sems.at[3]).wait()

    return pl.pallas_call(
        kernel,
        out_shape=[
            jax.ShapeDtypeStruct((n_row, CAP, width), table.dtype),
            jax.ShapeDtypeStruct((8, LANES), jnp.int32),
        ],
        in_specs=[VMEM, ANY],
        out_specs=[VMEM, VMEM],
        scratch_shapes=[
            pltpu.VMEM((2, cut, width), table.dtype),
            pltpu.VMEM((rows_local, width), jnp.float32),
            pltpu.VMEM((n_row, 1, LANES), jnp.int32),
            pltpu.SMEM((n_row, 1, LANES), jnp.int32),
            pltpu.VMEM((CAP, width), jnp.float32),
            pltpu.VMEM((n_row, CAP, width), table.dtype),
            pltpu.SemaphoreType.DMA((4,)),
            pltpu.SemaphoreType.DMA((2,)),
        ],
        compiler_params=params(),
    )(want, table)


def gather_cands(n_row, n_dp, my_cands, most):
    chunk, width = my_cands.shape

    def kernel(mine_ref, most_ref, all_ref, top_ref, theirs, sems):
        row, dp = lax.axis_index("row"), lax.axis_index("dp")
        other = lax.rem(dp + 1, n_dp)
        me = dp * n_row + row

        def one(j, carry):
            peer = lax.rem(row + j, n_row)
            pltpu.make_async_remote_copy(
                src_ref=mine_ref, dst_ref=all_ref.at[me], send_sem=sems.at[0], recv_sem=sems.at[1],
                device_id={"row": peer, "dp": dp}, device_id_type=MESH).start()
            return carry
        lax.fori_loop(1, n_row, one, 0)
        pltpu.make_async_copy(mine_ref, all_ref.at[me], sems.at[1]).start()
        count = pltpu.make_async_remote_copy(
            src_ref=most_ref, dst_ref=theirs, send_sem=sems.at[4], recv_sem=sems.at[5],
            device_id={"row": row, "dp": other}, device_id_type=MESH)
        count.start()
        half = all_ref.at[pl.ds(dp * n_row, n_row)]
        pltpu.make_async_copy(half, half, sems.at[1]).wait()
        swap = pltpu.make_async_remote_copy(
            src_ref=half, dst_ref=half, send_sem=sems.at[2], recv_sem=sems.at[3],
            device_id={"row": row, "dp": other}, device_id_type=MESH)
        swap.start()
        count.wait()
        top_ref[...] = jnp.maximum(most_ref[...], theirs[...])
        sent = all_ref.at[pl.ds(0, n_row - 1)]
        pltpu.make_async_copy(sent, sent, sems.at[0]).wait()
        swap.wait()

    return pl.pallas_call(
        kernel,
        out_shape=[
            jax.ShapeDtypeStruct((n_dp * n_row, chunk, width), my_cands.dtype),
            jax.ShapeDtypeStruct(most.shape, most.dtype),
        ],
        in_specs=[VMEM, VMEM],
        out_specs=[VMEM, VMEM],
        scratch_shapes=[pltpu.VMEM(most.shape, most.dtype), pltpu.SemaphoreType.DMA((6,))],
        compiler_params=params(),
    )(my_cands, most)


def softmax(n_total, cand_rows, hidden, tgt, y_lanes, cand_ids, log_q):
    n_cand, width = cand_rows.shape
    n_tok = hidden.shape[0]
    n_blk, n_sub = n_cand // BLK, n_tok // TOK
    f32 = jnp.float32

    def kernel(cands, h_ref, t_ref, y_ref, id_ref, lq_ref, cg_ref, dh_ref, dz_ref, loss_ref, z, g, h_t, acc, stat):
        h_t[...] = jnp.transpose(h_ref[...].astype(f32)).astype(jnp.bfloat16)
        for s in range(n_sub):
            tok = pl.ds(s * TOK, TOK)
            prod = h_ref[tok, :].astype(f32) * t_ref[tok, :].astype(f32)
            z_tgt = jnp.broadcast_to(jnp.sum(prod, axis=1, keepdims=True), (TOK, LANES))
            stat[0, tok, :] = z_tgt
            stat[1, tok, :] = z_tgt
        def logits(b, carry):
            rows = cands[pl.ds(pl.multiple_of(b * BLK, BLK), BLK), :]
            cols = pl.ds(pl.multiple_of(b * BLK, BLK), BLK)
            lq, cid = lq_ref[:, cols], id_ref[:, cols]

            def sub(s, c2):
                tok = pl.ds(pl.multiple_of(s * TOK, TOK), TOK)
                zz = lax.dot_general(h_ref[tok, :], rows, (((1,), (1,)), ((), ())), preferred_element_type=f32) - lq
                y = y_ref[tok, :]
                top = stat[1, tok, :]
                for k in range(BLK // LANES):
                    ln = slice(k * LANES, (k + 1) * LANES)
                    part = jnp.where(y == cid[:, ln], -1e9, zz[:, ln])
                    z[tok, pl.ds(pl.multiple_of(b * BLK + k * LANES, LANES), LANES)] = part
                    top = jnp.maximum(top, part)
                stat[1, tok, :] = top
                return c2
            return lax.fori_loop(0, n_sub, sub, carry)
        lax.fori_loop(0, n_blk, logits, 0)

        for s in range(n_sub):
            tok = pl.ds(s * TOK, TOK)
            stat[1, tok, :] = jnp.broadcast_to(jnp.max(stat[1, tok, :], axis=1, keepdims=True), (TOK, LANES))
            stat[2, tok, :] = jnp.zeros((TOK, LANES), f32)

        def exps(b, carry):
            def sub(s, c2):
                tok = pl.ds(pl.multiple_of(s * TOK, TOK), TOK)
                top = stat[1, tok, :]
                tot = stat[2, tok, :]
                for k in range(BLK // LANES):
                    at = pl.ds(pl.multiple_of(b * BLK + k * LANES, LANES), LANES)
                    e = jnp.exp(z[tok, at] - top)
                    z[tok, at] = e
                    tot = tot + e
                stat[2, tok, :] = tot
                return c2
            return lax.fori_loop(0, n_sub, sub, carry)
        lax.fori_loop(0, n_blk, exps, 0)

        loss_ref[...] = jnp.zeros_like(loss_ref)
        for s in range(n_sub):
            tok = pl.ds(s * TOK, TOK)
            z_tgt, top = stat[0, tok, :], stat[1, tok, :]
            e_tgt = jnp.exp(z_tgt - top)
            total = e_tgt + jnp.broadcast_to(jnp.sum(stat[2, tok, :], axis=1, keepdims=True), (TOK, LANES))
            dz = (e_tgt / total - 1.0) * (1.0 / n_total)
            dz_ref[tok, :] = dz
            stat[2, tok, :] = (1.0 / total) * (1.0 / n_total)
            part = top + jnp.log(total) - z_tgt
            loss_ref[...] += jnp.broadcast_to(jnp.sum(part, axis=0, keepdims=True), loss_ref.shape)
            acc[tok, :] = dz * t_ref[tok, :].astype(f32)

        def grads(b, carry):
            rows = cands[pl.ds(pl.multiple_of(b * BLK, BLK), BLK), :]

            def sub(s, c2):
                tok = pl.ds(pl.multiple_of(s * TOK, TOK), TOK)
                inv = stat[2, tok, :]
                for k in range(BLK // LANES):
                    at = pl.ds(pl.multiple_of(b * BLK + k * LANES, LANES), LANES)
                    g[tok, k * LANES:(k + 1) * LANES] = (z[tok, at] * inv).astype(jnp.bfloat16)
                acc[tok, :] += jnp.dot(g[tok, :], rows, preferred_element_type=f32)
                return c2
            lax.fori_loop(0, n_sub, sub, 0)
            cg_t = jnp.dot(h_t[...], g[...], preferred_element_type=f32)
            cg_ref[pl.ds(pl.multiple_of(b * BLK, BLK), BLK), :] = jnp.transpose(cg_t)
            return carry
        lax.fori_loop(0, n_blk, grads, 0)
        dh_ref[...] = acc[...].astype(jnp.bfloat16)

    return pl.pallas_call(
        kernel,
        out_shape=[
            jax.ShapeDtypeStruct((n_cand, width), f32),
            jax.ShapeDtypeStruct((n_tok, width), jnp.bfloat16),
            jax.ShapeDtypeStruct((n_tok, LANES), f32),
            jax.ShapeDtypeStruct((8, LANES), f32),
        ],
        in_specs=[VMEM] * 6,
        out_specs=[VMEM] * 4,
        scratch_shapes=[
            pltpu.VMEM((n_tok, n_cand), f32),
            pltpu.VMEM((n_tok, BLK), jnp.bfloat16),
            pltpu.VMEM((width, n_tok), jnp.bfloat16),
            pltpu.VMEM((n_tok, width), f32),
            pltpu.VMEM((3, n_tok, LANES), f32),
        ],
        compiler_params=pltpu.CompilerParams(vmem_limit_bytes=60 * 1024 * 1024),
    )(cand_rows, hidden, tgt, y_lanes, cand_ids, log_q)


def coords(row, side):
    return row // (side * side), lax.rem(row // side, side), lax.rem(row, side)


def order(part, z, y, x):
    return ((x, y, z), (y, z, x), (z, x, y))[part]


def row_of(part, a, b, c, side):
    z, y, x = ((c, b, a), (b, a, c), (a, c, b))[part]
    return (z * side + y) * side + x


def core_sum(side, cand, rest):
    n_row = side ** 3
    n_dp, rows = cand.shape[0], cand.shape[3]
    width = cand.shape[-1]

    def kernel(cand_ref, rest_ref, s0, s1, s2, cand_in, rest_in, sems):
        row, dp = lax.axis_index("row"), lax.axis_index("dp")
        other = lax.rem(dp + 1, n_dp)
        copies = [
            pltpu.make_async_remote_copy(
                src_ref=src.at[other], dst_ref=dst, send_sem=sems.at[i, 0], recv_sem=sems.at[i, 1],
                device_id={"row": row, "dp": other}, device_id_type=MESH)
            for i, (src, dst) in enumerate(((cand_ref, cand_in), (rest_ref, rest_in)))]
        for c in copies:
            c.start()
        for c in copies:
            c.wait()

        def one(r, carry):
            z, y, x = coords(r, side)
            a, b, c = order(0, z, y, x)
            s0[a, b, c] = cand_ref[dp, r, 0] + cand_in[r, 0]
            a, b, c = order(1, z, y, x)
            s1[a, b, c] = cand_ref[dp, r, 1] + cand_in[r, 1]
            a, b, c = order(2, z, y, x)
            s2[a, b, c] = rest_ref[dp, r] + rest_in[r]
            return carry
        lax.fori_loop(0, n_row, one, 0)

    lead = (side, side, side)
    return pl.pallas_call(
        kernel,
        out_shape=[jax.ShapeDtypeStruct(lead + (n, width), jnp.float32) for n in (rows, rows, rest.shape[2])],
        in_specs=[VMEM, VMEM],
        out_specs=[VMEM] * 3,
        scratch_shapes=[
            pltpu.VMEM(cand.shape[1:], jnp.float32),
            pltpu.VMEM(rest.shape[1:], jnp.float32),
            pltpu.SemaphoreType.DMA((2, 2)),
        ],
        compiler_params=params(),
    )(cand, rest)


def axis_sum(side, parts, moved):
    n_row = side ** 3
    n_p, n_m = len(parts), len(moved)
    f32 = jnp.float32

    def kernel(*refs):
        refs = list(refs)
        take = lambda n: [refs.pop(0) for _ in range(n)]
        s, out = take(n_p), take(n_m)
        g, into = take(n_p), take(n_m)
        r1, t1, r2, t2, r3 = (take(n_p) for _ in range(5))
        sems, m_sems = refs
        row, dp = lax.axis_index("row"), lax.axis_index("dp")
        z, y, x = coords(row, side)
        at = [order(p, z, y, x) for p in range(n_p)]

        def send(p, phase, axis, k, src, dst):
            to = list(at[p])
            to[axis] = lax.rem(to[axis] + k, side)
            pltpu.make_async_remote_copy(
                src_ref=src(to[axis]), dst_ref=dst, send_sem=sems.at[p, phase, 0], recv_sem=sems.at[p, phase, 1],
                device_id={"row": row_of(p, *to, side), "dp": dp}, device_id_type=MESH).start()

        def wait(p, phase, d, like):
            pltpu.make_async_copy(like, like, sems.at[p, phase, d]).wait()

        def move(lo, hi):
            def one(j, carry):
                peer = lax.rem(row + j, n_row)
                for i in range(n_m):
                    pltpu.make_async_remote_copy(
                        src_ref=out[i].at[peer], dst_ref=into[i].at[row], send_sem=m_sems.at[i, 0], recv_sem=m_sems.at[i, 1],
                        device_id={"row": peer, "dp": dp}, device_id_type=MESH).start()
                return carry
            lax.fori_loop(lo, hi, one, 0)
        cuts = [1 + (n_row - 1) * i // 6 for i in range(7)]

        src_of = (s, t1, t2)
        got_of = (r1, r2, r3)
        sum_of = (t1, t2, None)
        for phase in range(3):
            for p in range(n_p):
                for k in range(1, side):
                    send(p, phase, phase, k, lambda i, p=p: src_of[phase][p].at[i], got_of[phase][p].at[at[p][phase]])
            move(cuts[phase], cuts[phase + 1])
            if phase == 0:
                for i in range(n_m):
                    pltpu.make_async_copy(out[i].at[row], into[i].at[row], m_sems.at[i, 1]).start()
            for p in range(n_p):
                mine, got = src_of[phase][p], got_of[phase][p]
                wait(p, phase, 1, got.at[pl.ds(0, side - 1)])
                me = at[p][phase]

                def total(idx, p=p, mine=mine, got=got, me=me):
                    v = mine[(me,) + idx]
                    for k in range(1, side):
                        v = v + got[(lax.rem(me + k, side),) + idx]
                    return v
                if phase == 0:
                    def body(i, carry, p=p, total=total):
                        for j in range(side):
                            t1[p][i, j] = total((i, j))
                        return carry
                    lax.fori_loop(0, side, body, 0)
                elif phase == 1:
                    def body(i, carry, p=p, total=total):
                        t2[p][i] = total((i,))
                        return carry
                    lax.fori_loop(0, side, body, 0)
                else:
                    g[p][at[p][0], at[p][1], at[p][2]] = total(())

        for phase in range(3, 6):
            axis = 5 - phase
            for p in range(n_p):
                blk = g[p].at[at[p][:axis + 1]]
                for k in range(1, side):
                    send(p, phase, axis, k, lambda i, blk=blk: blk, blk)
            move(cuts[phase], cuts[phase + 1])
            for p in range(n_p):
                wait(p, phase, 1, g[p].at[at[p][:axis] + (pl.ds(0, side - 1),)])
        for p in range(n_p):
            for phase in range(3):
                wait(p, phase, 0, src_of[phase][p].at[pl.ds(0, side - 1)])
                axis = 2 - phase
                wait(p, phase + 3, 0, g[p].at[at[p][:axis] + (pl.ds(0, side - 1),)])
        for i in range(n_m):
            sent = out[i].at[pl.ds(0, n_row - 1)]
            pltpu.make_async_copy(sent, sent, m_sems.at[i, 0]).wait()
            pltpu.make_async_copy(into[i], into[i], m_sems.at[i, 1]).wait()

    same = [jax.ShapeDtypeStruct(v.shape, v.dtype) for v in list(parts) + list(moved)]
    scratch = [[pltpu.VMEM(shape(v.shape), f32) for v in parts] for shape in (
        lambda q: q, lambda q: q[1:], lambda q: q[1:], lambda q: q[2:], lambda q: q[2:])]
    return pl.pallas_call(
        kernel,
        out_shape=same,
        in_specs=[VMEM] * len(same),
        out_specs=[VMEM] * len(same),
        scratch_shapes=[v for group in scratch for v in group] + [
            pltpu.SemaphoreType.DMA((n_p, 6, 2)), pltpu.SemaphoreType.DMA((n_m, 2))],
        compiler_params=params(),
    )(*parts, *moved)


def core_swap(n_dp, *xs):
    n = len(xs)

    def kernel(*refs):
        ins, outs, sems = refs[:n], refs[n:2 * n], refs[2 * n]
        row, dp = lax.axis_index("row"), lax.axis_index("dp")
        other = lax.rem(dp + 1, n_dp)
        copies = []
        for i in range(n):
            copies.append(pltpu.make_async_remote_copy(
                src_ref=ins[i], dst_ref=outs[i].at[dp], send_sem=sems.at[i, 0], recv_sem=sems.at[i, 1],
                device_id={"row": row, "dp": other}, device_id_type=MESH))
            copies.append(pltpu.make_async_copy(ins[i], outs[i].at[dp], sems.at[i, 2]))
        for c in copies:
            c.start()
        for c in copies:
            c.wait()

    return pl.pallas_call(
        kernel,
        out_shape=[jax.ShapeDtypeStruct((n_dp,) + x.shape, x.dtype) for x in xs],
        in_specs=[VMEM] * n,
        out_specs=[VMEM] * n,
        scratch_shapes=[pltpu.SemaphoreType.DMA((n, 3))],
        compiler_params=params(),
    )(*xs)


def add_rows(n_rows, groups, grad=None, n_acc=4):
    width = groups[0][2].shape[1]
    n_full = n_rows + 8
    chunk = min(128, n_rows)
    flat, specs = [], []
    for row_ids, counts, vals, val_ids in groups:
        flat += [row_ids, counts, vals] + ([] if val_ids is None else [val_ids])
        specs += [SMEM, SMEM, VMEM] + ([] if val_ids is None else [SMEM])
    if grad is not None:
        flat.append(grad)
        specs.append(ANY)

    def kernel(*refs):
        refs = list(refs)
        work = []
        for _, _, vals, val_ids in groups:
            idx, cnt, ref = refs.pop(0), refs.pop(0), refs.pop(0)
            work.append((idx, cnt, ref, None if val_ids is None else refs.pop(0)))
        grad_ref = refs.pop(0) if grad is not None else None
        out_ref, sem = refs[0], refs[-1]
        accs = refs[1:-1]
        if grad_ref is not None:
            cp_in = pltpu.make_async_copy(grad_ref, accs[0].at[pl.ds(0, n_rows)], sem)
            cp_in.start()
        fresh = accs if grad_ref is None else accs[1:]

        def clear(k, carry):
            for a in fresh:
                a[pl.ds(pl.multiple_of(k * chunk, chunk), chunk), :] = jnp.zeros((chunk, width), jnp.float32)
            return carry
        if fresh:
            lax.fori_loop(0, n_rows // chunk, clear, 0)
        for a in accs:
            a[pl.ds(n_rows, 8), :] = jnp.zeros((8, width), jnp.float32)
        if grad_ref is not None:
            cp_in.wait()

        for idx, cnt, vals_ref, vid in work:
            per_list = vals_ref.shape[0] // idx.shape[0]

            def one_list(i, carry, idx=idx, cnt=cnt, vals_ref=vals_ref, vid=vid, per_list=per_list):
                def group(q, c2):
                    for u in range(8):
                        c = q * 8 + u
                        acc = accs[u % n_acc]
                        r = idx[i, c]
                        v = i * per_list + c if vid is None else vid[i, c]
                        acc[pl.ds(r, 1), :] += vals_ref[pl.ds(v, 1), :]
                    return c2
                return lax.fori_loop(0, (cnt[i] + 7) // 8, group, carry)
            lax.fori_loop(0, idx.shape[0], one_list, 0)

        if n_acc > 1:
            def merge(k, carry):
                sl = pl.ds(pl.multiple_of(k * chunk, chunk), chunk)
                tot = accs[0][sl, :]
                for a in accs[1:]:
                    tot = tot + a[sl, :]
                accs[0][sl, :] = tot
                return carry
            lax.fori_loop(0, n_rows // chunk, merge, 0)
        cp_out = pltpu.make_async_copy(accs[0].at[pl.ds(0, n_rows)], out_ref, sem)
        cp_out.start()
        cp_out.wait()

    return pl.pallas_call(
        kernel,
        out_shape=jax.ShapeDtypeStruct((n_rows, width), jnp.float32),
        in_specs=specs,
        out_specs=ANY,
        scratch_shapes=[pltpu.VMEM((n_full, width), jnp.float32)] * n_acc + [pltpu.SemaphoreType.DMA],
        compiler_params=pltpu.CompilerParams(vmem_limit_bytes=60 * 1024 * 1024),
    )(*flat)


def ranks(owner, n_row):
    n = owner.shape[0]
    hot = (owner[:, None] == jnp.arange(n_row)[None, :]).astype(jnp.bfloat16)
    pos = jnp.arange(n)
    before = (pos[:, None] > pos[None, :]).astype(jnp.bfloat16)
    earlier = jnp.dot(before, hot, preferred_element_type=jnp.float32)
    hot32 = hot.astype(jnp.float32)
    return jnp.sum(earlier * hot32, axis=1).astype(jnp.int32), jnp.sum(hot32, axis=0).astype(jnp.int32)


def to_slots(slot, vals, n_slots):
    hit = slot[:, None] == jnp.arange(n_slots)[None, :]
    return [jnp.sum(jnp.where(hit, v[:, None], jnp.zeros((), v.dtype)), axis=0) for v in vals]


def tile_rows(rows, n_row):
    padded = [jnp.pad(r, ((0, 0), (0, LANES - r.shape[1]))) for r in rows]
    padded += [jnp.zeros_like(padded[0])] * (8 - len(rows))
    return jnp.stack(padded, axis=1)


def solution(mesh):
    n_row, n_dp = mesh.shape["row"], mesh.shape["dp"]
    n_dev = n_row * n_dp
    side = round(n_row ** (1 / 3))

    def run_step(x_tok, w_up, w_down, item_table, cand_ids, log_q, targets):
        n_total = x_tok.shape[0]

        def device_step(x_loc, w_up, w_down, tab_loc, cand_ids, log_q, y_loc):
            rows_local, width = tab_loc.shape
            n_tok = y_loc.shape[0]
            n_cand = cand_ids.shape[0]
            row, dp = lax.axis_index("row"), lax.axis_index("dp")
            me = dp * n_row + row
            chunk = n_cand // n_dev
            f32, bf16 = jnp.float32, jnp.bfloat16
            n_ids = n_tok + chunk
            n_pad = -(-n_ids // LANES) * LANES

            my_cands = lax.dynamic_slice_in_dim(cand_ids, me * chunk, chunk)
            ids = jnp.concatenate([y_loc, my_cands])
            owner, local = ids // rows_local, ids % rows_local
            rank, per_owner = ranks(owner, n_row)
            most = jnp.max(per_owner)

            pre_act = jnp.dot(x_loc, w_up, preferred_element_type=f32)
            act_full, gelu_vjp = jax.vjp(jax.nn.gelu, pre_act)
            act_b = act_full.astype(bf16)
            hidden = jnp.dot(act_b, w_down, preferred_element_type=f32).astype(bf16)

            split = jnp.pad(jnp.stack([local // 128, local % 128], axis=1).astype(bf16), ((0, n_pad - n_ids), (0, LANES - 2)))
            carried = jnp.concatenate([jnp.pad(hidden, ((0, n_pad - n_tok), (0, 0))), split], axis=1)

            def pack_round(k):
                rel = rank - k * CAP
                hit = (rel >= 0) & (rel < CAP)
                slot = jnp.where(hit, owner * LANES + rel, -1)
                hid_out, want = pack(jnp.pad(slot, (0, n_pad - n_ids), constant_values=-1)[None, :], carried, n_row)
                return hit, owner * CAP + rel, hid_out, want

            def fetch_round(k):
                hit, at, hid_out, want = pack_round(k)
                lane = jnp.arange(LANES)[None, None, :]
                rows_in, most_all = fetch(n_row, n_dp, jnp.where(lane == LANES - 1, most, want), tab_loc)
                got = jnp.take(rows_in.reshape(n_row * CAP, width), at, axis=0, mode="clip")
                return hit, got, hid_out, most_all

            _, got, hid_out, most_dp = fetch_round(0)
            cand_rows, most_all = gather_cands(n_row, n_dp, got[n_tok:], most_dp)
            most_all = most_all[0, LANES - 1]

            def fetch_more(carry):
                k, got, _ = carry
                hit, new, _, most = fetch_round(k)
                got = jnp.where(hit[:, None], new, got)
                return k + 1, got, gather_cands(n_row, n_dp, got[n_tok:], most)[0]

            _, got, cand_rows = lax.while_loop(
                lambda c: c[0] * CAP < most_all, fetch_more, (jnp.int32(1), got, cand_rows))
            tgt_rows, cand_rows = got[:n_tok], cand_rows.reshape(n_cand, width)

            cand_grad, grad_hid, dz_lanes, loss_part = softmax(
                n_total, cand_rows, hidden, tgt_rows,
                jnp.broadcast_to(y_loc[:, None], (n_tok, LANES)), cand_ids[None, :], log_q[None, :])
            dz_tgt, loss_sum = dz_lanes[:, 0], loss_part[0, 0]

            grad_down = jnp.einsum("tf,td->fd", act_b, grad_hid, preferred_element_type=f32)
            grad_act = jnp.einsum("td,fd->tf", grad_hid, w_down, preferred_element_type=f32)
            grad_pre = gelu_vjp(grad_act)[0].astype(bf16)
            grad_up = jnp.einsum("ti,tf->if", x_loc, grad_pre, preferred_element_type=f32)

            t_rank, t_owner, t_local = rank[:n_tok], owner[:n_tok], local[:n_tok]
            t_count = jnp.sum((t_owner[:, None] == jnp.arange(n_row)[None, :]).astype(jnp.int32), axis=0)
            c_rank, _ = ranks(owner[n_tok:], n_row)
            c_slot = owner[n_tok:] * chunk + c_rank
            c_count = per_owner - t_count
            c_row, c_pos = to_slots(c_slot, [(local[n_tok:] - rows_local).astype(f32), jnp.arange(chunk, dtype=f32)], n_row * chunk)
            c_row = (c_row + rows_local).reshape(n_row, chunk)
            c_pos = c_pos.reshape(n_row, chunk)
            half, z_y_x = chunk // 2, coords(row, side)
            first = []
            for part in range(2):
                a, b, c = order(part, *z_y_x)
                first.append((((part * n_dp + dp) * n_row + (a * side + b) * side + c) * half).astype(f32))
            c_pos = jnp.where(c_pos < half, first[0] + c_pos, first[1] + c_pos - half)

            def give(k):
                rel = t_rank - k * CAP
                slot = jnp.where((rel >= 0) & (rel < CAP), t_owner * CAP + rel, -1)
                t_row, t_dz = to_slots(slot, [t_local.astype(f32), dz_tgt], n_row * CAP)
                now = jnp.clip(t_count - k * CAP, 0, CAP).astype(f32)
                counts = jnp.stack([now, c_count.astype(f32), jnp.full((n_row,), loss_sum)], axis=1)
                return tile_rows([t_row.reshape(n_row, CAP), t_dz.reshape(n_row, CAP), c_row, c_pos, counts], n_row)

            to_int = lambda v: v.astype(jnp.int32)

            def token_group(hid_in, meta_in):
                vals = meta_in[:, 1, :CAP, None] * hid_in.astype(f32)
                return to_int(meta_in[:, 0, :CAP]), to_int(meta_in[:, 4, 0]), vals.reshape(n_dev * CAP, width), None

            blocks = w_up.shape[1] // LANES
            up_shape = (n_dev // blocks, w_up.shape[0] * blocks // n_dev, blocks, LANES)
            rest = jnp.concatenate([
                grad_up.reshape(up_shape).transpose(0, 2, 1, 3).reshape(n_dp, n_row, up_shape[1], width),
                grad_down.reshape(n_dp, n_row, -1, width)], axis=2)
            parts = core_sum(side, cand_grad.reshape(n_dp, n_row, 2, half, width), rest)
            g0, g1, g2, hid_in, meta_in = axis_sum(side, parts, [hid_out, give(0)])
            g0, g1, g2, hid_in, meta_in = core_swap(n_dp, g0, g1, g2, hid_in, meta_in)
            hid_in, meta_in = hid_in.reshape(n_dev, CAP, width), meta_in.reshape(n_dev, 8, LANES)
            cand_sums = jnp.concatenate([g0.reshape(-1, width), g1.reshape(-1, width)], axis=0)
            rest = jnp.transpose(g2, (0, 1, 3, 2, 4, 5)).reshape(n_dev, -1, width)
            grad_up = rest[:, :up_shape[1]].reshape(up_shape[0], blocks, up_shape[1], LANES).transpose(0, 2, 1, 3).reshape(w_up.shape)
            grad_down = rest[:, up_shape[1]:].reshape(w_down.shape)

            grad = add_rows(rows_local, [
                token_group(hid_in, meta_in),
                (to_int(meta_in[:, 2, :chunk]), to_int(meta_in[:, 4, 1]), cand_sums, to_int(meta_in[:, 3, :chunk]))])

            def give_more(carry):
                k, grad = carry
                return k + 1, add_rows(rows_local, [token_group(*exchange(n_row, n_dp, True, pack_round(k)[2], give(k)))], grad, 1)

            _, grad = lax.while_loop(lambda c: c[0] * CAP < most_all, give_more, (jnp.int32(1), grad))
            return jnp.sum(meta_in[:, 4, 2]) / n_total, grad, grad_up, grad_down

        return jax.shard_map(
            device_step,
            mesh=mesh,
            in_specs=(P(ALL_AXES, None), P(), P(), P("row", None), P(), P(), P(ALL_AXES)),
            out_specs=(P(), P("row", None), P(), P()),
            check_vma=False,
        )(x_tok, w_up, w_down, item_table, cand_ids, log_q, targets)

    return run_step
```

```python
import functools

import jax
import jax.numpy as jnp
from jax import lax
from jax.experimental import pallas as pl
from jax.experimental.pallas import tpu as pltpu
from jax.sharding import PartitionSpec as P

ALL_AXES = ("dp", "row")
MESH = pl.DeviceIdType.MESH
CAP = 112
BLK = 2048
TOK = 512
LANES = 128
ANY = pl.BlockSpec(memory_space=pl.ANY)
VMEM = pl.BlockSpec(memory_space=pltpu.VMEM)
SMEM = pl.BlockSpec(memory_space=pltpu.SMEM)


def params(barrier=None):
    return pltpu.CompilerParams(has_side_effects=True, vmem_limit_bytes=60 * 1024 * 1024, collective_id=barrier)


def greet(n_row, n_dp, rows, partner):
    row, dp = lax.axis_index("row"), lax.axis_index("dp")
    barrier = pltpu.get_barrier_semaphore()
    if partner:
        pl.semaphore_signal(barrier, inc=1, device_id={"row": row, "dp": lax.rem(dp + 1, n_dp)}, device_id_type=MESH)
    if rows:
        def one(j, carry):
            pl.semaphore_signal(barrier, inc=1, device_id={"row": lax.rem(row + j, n_row), "dp": dp}, device_id_type=MESH)
            return carry
        lax.fori_loop(1, n_row, one, 0)
    pl.semaphore_wait(barrier, (n_row - 1 if rows else 0) + (1 if partner else 0))


def exchange(n_row, n_dp, both, *xs):
    n_x = len(xs)
    steps = range(n_dp) if both else range(1)
    n_out = n_row * (n_dp if both else 1)

    def kernel(*refs):
        ins, outs = refs[:n_x], refs[n_x:2 * n_x]
        send_sem, recv_sem = refs[2 * n_x:]
        row, dp = lax.axis_index("row"), lax.axis_index("dp")
        slot = dp * n_row + row if both else row
        for i in range(n_x):
            pltpu.make_async_copy(ins[i].at[row], outs[i].at[slot], recv_sem.at[i]).start()

        for e in steps:
            def send(j, carry, e=e):
                peer = lax.rem(row + j, n_row)
                for i in range(n_x):
                    pltpu.make_async_remote_copy(
                        src_ref=ins[i].at[peer],
                        dst_ref=outs[i].at[slot],
                        send_sem=send_sem.at[i, e],
                        recv_sem=recv_sem.at[i],
                        device_id={"row": peer, "dp": lax.rem(dp + e, n_dp)},
                        device_id_type=MESH,
                    ).start()
                return carry
            lax.fori_loop(0 if e else 1, n_row, send, 0)
        for i in range(n_x):
            for e in steps:
                sent = ins[i] if e else ins[i].at[pl.ds(0, n_row - 1)]
                pltpu.make_async_copy(sent, sent, send_sem.at[i, e]).wait()
            pltpu.make_async_copy(outs[i], outs[i], recv_sem.at[i]).wait()

    return pl.pallas_call(
        kernel,
        out_shape=[jax.ShapeDtypeStruct((n_out,) + x.shape[1:], x.dtype) for x in xs],
        in_specs=[VMEM] * n_x,
        out_specs=[VMEM] * n_x,
        scratch_shapes=[pltpu.SemaphoreType.DMA((n_x, n_dp)), pltpu.SemaphoreType.DMA((n_x,))],
        compiler_params=params(),
    )(*xs)


def pack(slot_row, vals, n_row):
    n_pad = slot_row.shape[1]
    per = 4 if n_row % 4 == 0 else 1

    def kernel(slot_ref, vals_ref, hid_ref, want_ref):
        base = pl.program_id(0) * (per * LANES)
        at = lax.broadcasted_iota(jnp.int32, (per * LANES, n_pad), 0) + base
        hit = (at == slot_ref[...]).astype(jnp.float32).astype(jnp.bfloat16)
        got = jnp.dot(hit, vals_ref[...], preferred_element_type=jnp.float32)
        for o in range(per):
            blk = got[o * LANES:(o + 1) * LANES]
            hid_ref[o] = blk[:CAP, :LANES].astype(jnp.bfloat16)
            ids = jnp.transpose(blk[:, LANES:])
            want_ref[o] = (ids[0:1] * 128.0 + ids[1:2]).astype(jnp.int32)

    return pl.pallas_call(
        kernel,
        grid=(n_row // per,),
        out_shape=[
            jax.ShapeDtypeStruct((n_row, CAP, LANES), jnp.bfloat16),
            jax.ShapeDtypeStruct((n_row, 1, LANES), jnp.int32),
        ],
        in_specs=[pl.BlockSpec((1, n_pad), lambda i: (0, 0)), pl.BlockSpec((n_pad, 2 * LANES), lambda i: (0, 0))],
        out_specs=[
            pl.BlockSpec((per, CAP, LANES), lambda i: (i, 0, 0)),
            pl.BlockSpec((per, 1, LANES), lambda i: (i, 0, 0)),
        ],
        compiler_params=pltpu.CompilerParams(vmem_limit_bytes=40 * 1024 * 1024),
    )(slot_row, vals)


def fetch(n_row, n_dp, want, table):
    rows_local, width = table.shape
    cut = min(1024, rows_local // 2)
    n_cut = rows_local // cut

    def kernel(want_ref, tab_ref, rows_ref, most_ref, tab16, tab32, asked, ask_s, stage, out_buf, sems, tab_sem):
        row, dp = lax.axis_index("row"), lax.axis_index("dp")

        def load(k, p):
            sl = pl.ds(pl.multiple_of(k * cut, cut), cut)
            return pltpu.make_async_copy(tab_ref.at[sl], tab16.at[p], tab_sem.at[p])
        load(0, 0).start()
        load(1, 1).start()
        greet(n_row, n_dp, True, False)
        pltpu.make_async_copy(want_ref.at[row], asked.at[row], sems.at[1]).start()

        def ask(j, carry):
            peer = lax.rem(row + j, n_row)
            pltpu.make_async_remote_copy(
                src_ref=want_ref.at[peer], dst_ref=asked.at[row], send_sem=sems.at[0], recv_sem=sems.at[1],
                device_id={"row": peer, "dp": dp}, device_id_type=MESH).start()
            return carry
        lax.fori_loop(1, n_row, ask, 0)

        def widen(k, more):
            for p in range(2):
                load(2 * k + p, p).wait()
                sl = pl.ds(pl.multiple_of((2 * k + p) * cut, cut), cut)
                tab32[sl, :] = tab16[p].astype(jnp.float32)
                if more:
                    load(2 * k + p + 2, p).start()
            return 0
        lax.fori_loop(0, n_cut // 2 - 1, lambda k, c: widen(k, True), 0)
        widen(n_cut // 2 - 1, False)
        pltpu.make_async_copy(asked, asked, sems.at[1]).wait()
        to_s = pltpu.make_async_copy(asked, ask_s, tab_sem.at[0])
        to_s.start()
        most_ref[...] = jnp.broadcast_to(jnp.max(asked[...], axis=0), (8, LANES))
        to_s.wait()

        def send(peer):
            pltpu.make_async_remote_copy(
                src_ref=out_buf.at[peer], dst_ref=rows_ref.at[row], send_sem=sems.at[2], recv_sem=sems.at[3],
                device_id={"row": peer, "dp": dp}, device_id_type=MESH).start()

        def gather(j):
            peer = lax.rem(row + j, n_row)
            for c in range(CAP):
                stage[pl.ds(c, 1), :] = tab32[pl.ds(ask_s[peer, 0, c], 1), :]
            out_buf[peer] = stage[...].astype(jnp.bfloat16)

        def step(j, carry):
            gather(j)

            @pl.when(j > 1)
            def _():
                send(lax.rem(row + j - 1, n_row))
            return carry
        lax.fori_loop(1, n_row + 1, step, 0)
        pltpu.make_async_copy(out_buf.at[row], rows_ref.at[row], sems.at[3]).start()
        sent = want_ref.at[pl.ds(0, n_row - 1)]
        pltpu.make_async_copy(sent, sent, sems.at[0]).wait()
        sent = out_buf.at[pl.ds(0, n_row - 1)]
        pltpu.make_async_copy(sent, sent, sems.at[2]).wait()
        pltpu.make_async_copy(rows_ref, rows_ref, sems.at[3]).wait()

    return pl.pallas_call(
        kernel,
        out_shape=[
            jax.ShapeDtypeStruct((n_row, CAP, width), table.dtype),
            jax.ShapeDtypeStruct((8, LANES), jnp.int32),
        ],
        in_specs=[VMEM, ANY],
        out_specs=[VMEM, VMEM],
        scratch_shapes=[
            pltpu.VMEM((2, cut, width), table.dtype),
            pltpu.VMEM((rows_local, width), jnp.float32),
            pltpu.VMEM((n_row, 1, LANES), jnp.int32),
            pltpu.SMEM((n_row, 1, LANES), jnp.int32),
            pltpu.VMEM((CAP, width), jnp.float32),
            pltpu.VMEM((n_row, CAP, width), table.dtype),
            pltpu.SemaphoreType.DMA((4,)),
            pltpu.SemaphoreType.DMA((2,)),
        ],
        compiler_params=params(2),
    )(want, table)


def gather_cands(n_row, n_dp, got, n_tok, most):
    chunk, width = got.shape[0] - n_tok, got.shape[1]

    def kernel(got_ref, most_ref, all_ref, top_ref, theirs, sems):
        mine_ref = got_ref.at[pl.ds(n_tok, chunk)]
        row, dp = lax.axis_index("row"), lax.axis_index("dp")
        other = lax.rem(dp + 1, n_dp)
        me = dp * n_row + row

        greet(n_row, n_dp, True, True)

        def one(j, carry):
            peer = lax.rem(row + j, n_row)
            pltpu.make_async_remote_copy(
                src_ref=mine_ref, dst_ref=all_ref.at[me], send_sem=sems.at[0], recv_sem=sems.at[1],
                device_id={"row": peer, "dp": dp}, device_id_type=MESH).start()
            return carry
        lax.fori_loop(1, n_row, one, 0)
        pltpu.make_async_copy(mine_ref, all_ref.at[me], sems.at[1]).start()
        count = pltpu.make_async_remote_copy(
            src_ref=most_ref, dst_ref=theirs, send_sem=sems.at[4], recv_sem=sems.at[5],
            device_id={"row": row, "dp": other}, device_id_type=MESH)
        count.start()
        half = all_ref.at[pl.ds(dp * n_row, n_row)]
        pltpu.make_async_copy(half, half, sems.at[1]).wait()
        swap = pltpu.make_async_remote_copy(
            src_ref=half, dst_ref=half, send_sem=sems.at[2], recv_sem=sems.at[3],
            device_id={"row": row, "dp": other}, device_id_type=MESH)
        swap.start()
        count.wait()
        top_ref[...] = jnp.maximum(most_ref[...], theirs[...])
        sent = all_ref.at[pl.ds(0, n_row - 1)]
        pltpu.make_async_copy(sent, sent, sems.at[0]).wait()
        swap.wait()

    return pl.pallas_call(
        kernel,
        out_shape=[
            jax.ShapeDtypeStruct((n_dp * n_row, chunk, width), got.dtype),
            jax.ShapeDtypeStruct(most.shape, most.dtype),
        ],
        in_specs=[VMEM, VMEM],
        out_specs=[VMEM, VMEM],
        scratch_shapes=[pltpu.VMEM(most.shape, most.dtype), pltpu.SemaphoreType.DMA((6,))],
        compiler_params=params(3),
    )(got, most)


def softmax(n_total, cand_rows, hidden, tgt, y_lanes, cand_ids, log_q):
    n_cand, width = cand_rows.shape
    n_tok = hidden.shape[0]
    n_blk, n_sub = n_cand // BLK, n_tok // TOK
    f32 = jnp.float32

    def kernel(cands, h_ref, t_ref, y_ref, id_ref, lq_ref, cg_ref, dh_ref, dz_ref, loss_ref, z, g, h_t, acc, stat):
        h_t[...] = jnp.transpose(h_ref[...].astype(f32)).astype(jnp.bfloat16)
        for s in range(n_sub):
            tok = pl.ds(s * TOK, TOK)
            prod = h_ref[tok, :].astype(f32) * t_ref[tok, :].astype(f32)
            z_tgt = jnp.broadcast_to(jnp.sum(prod, axis=1, keepdims=True), (TOK, LANES))
            stat[0, tok, :] = z_tgt
            stat[1, tok, :] = z_tgt
        def logits(b, carry):
            rows = cands[pl.ds(pl.multiple_of(b * BLK, BLK), BLK), :]
            cols = pl.ds(pl.multiple_of(b * BLK, BLK), BLK)
            lq, cid = lq_ref[:, cols], id_ref[:, cols]

            def sub(s, c2):
                tok = pl.ds(pl.multiple_of(s * TOK, TOK), TOK)
                zz = lax.dot_general(h_ref[tok, :], rows, (((1,), (1,)), ((), ())), preferred_element_type=f32) - lq
                y = y_ref[tok, :]
                top = stat[1, tok, :]
                for k in range(BLK // LANES):
                    ln = slice(k * LANES, (k + 1) * LANES)
                    part = jnp.where(y == cid[:, ln], -1e9, zz[:, ln])
                    z[tok, pl.ds(pl.multiple_of(b * BLK + k * LANES, LANES), LANES)] = part
                    top = jnp.maximum(top, part)
                stat[1, tok, :] = top
                return c2
            return lax.fori_loop(0, n_sub, sub, carry)
        lax.fori_loop(0, n_blk, logits, 0)

        for s in range(n_sub):
            tok = pl.ds(s * TOK, TOK)
            stat[1, tok, :] = jnp.broadcast_to(jnp.max(stat[1, tok, :], axis=1, keepdims=True), (TOK, LANES))
            stat[2, tok, :] = jnp.zeros((TOK, LANES), f32)

        def exps(b, carry):
            def sub(s, c2):
                tok = pl.ds(pl.multiple_of(s * TOK, TOK), TOK)
                top = stat[1, tok, :]
                tot = stat[2, tok, :]
                for k in range(BLK // LANES):
                    at = pl.ds(pl.multiple_of(b * BLK + k * LANES, LANES), LANES)
                    e = jnp.exp(z[tok, at] - top)
                    z[tok, at] = e
                    tot = tot + e
                stat[2, tok, :] = tot
                return c2
            return lax.fori_loop(0, n_sub, sub, carry)
        lax.fori_loop(0, n_blk, exps, 0)

        loss_ref[...] = jnp.zeros_like(loss_ref)
        for s in range(n_sub):
            tok = pl.ds(s * TOK, TOK)
            z_tgt, top = stat[0, tok, :], stat[1, tok, :]
            e_tgt = jnp.exp(z_tgt - top)
            total = e_tgt + jnp.broadcast_to(jnp.sum(stat[2, tok, :], axis=1, keepdims=True), (TOK, LANES))
            dz = (e_tgt / total - 1.0) * (1.0 / n_total)
            dz_ref[tok, :] = dz
            stat[2, tok, :] = (1.0 / total) * (1.0 / n_total)
            part = top + jnp.log(total) - z_tgt
            loss_ref[...] += jnp.broadcast_to(jnp.sum(part, axis=0, keepdims=True), loss_ref.shape)
            acc[tok, :] = dz * t_ref[tok, :].astype(f32)

        def grads(b, carry):
            rows = cands[pl.ds(pl.multiple_of(b * BLK, BLK), BLK), :]

            def sub(s, c2):
                tok = pl.ds(pl.multiple_of(s * TOK, TOK), TOK)
                inv = stat[2, tok, :]
                for k in range(BLK // LANES):
                    at = pl.ds(pl.multiple_of(b * BLK + k * LANES, LANES), LANES)
                    g[tok, k * LANES:(k + 1) * LANES] = (z[tok, at] * inv).astype(jnp.bfloat16)
                acc[tok, :] += jnp.dot(g[tok, :], rows, preferred_element_type=f32)
                return c2
            lax.fori_loop(0, n_sub, sub, 0)
            cg_t = jnp.dot(h_t[...], g[...], preferred_element_type=f32)
            cg_ref[pl.ds(pl.multiple_of(b * BLK, BLK), BLK), :] = jnp.transpose(cg_t)
            return carry
        lax.fori_loop(0, n_blk, grads, 0)
        dh_ref[...] = acc[...].astype(jnp.bfloat16)

    return pl.pallas_call(
        kernel,
        out_shape=[
            jax.ShapeDtypeStruct((n_cand, width), f32),
            jax.ShapeDtypeStruct((n_tok, width), jnp.bfloat16),
            jax.ShapeDtypeStruct((n_tok, LANES), f32),
            jax.ShapeDtypeStruct((8, LANES), f32),
        ],
        in_specs=[VMEM] * 6,
        out_specs=[VMEM] * 4,
        scratch_shapes=[
            pltpu.VMEM((n_tok, n_cand), f32),
            pltpu.VMEM((n_tok, BLK), jnp.bfloat16),
            pltpu.VMEM((width, n_tok), jnp.bfloat16),
            pltpu.VMEM((n_tok, width), f32),
            pltpu.VMEM((3, n_tok, LANES), f32),
        ],
        compiler_params=pltpu.CompilerParams(vmem_limit_bytes=60 * 1024 * 1024),
    )(cand_rows, hidden, tgt, y_lanes, cand_ids, log_q)


def coords(row, side):
    return row // (side * side), lax.rem(row // side, side), lax.rem(row, side)


def order(part, z, y, x):
    return ((x, y, z), (y, z, x), (z, x, y))[part]


def row_of(part, a, b, c, side):
    z, y, x = ((c, b, a), (b, a, c), (a, c, b))[part]
    return (z * side + y) * side + x


def core_sum(side, cand, rest):
    n_row = side ** 3
    n_dp, rows = cand.shape[0], cand.shape[3]
    width = cand.shape[-1]

    def kernel(cand_ref, rest_ref, s0, s1, s2, cand_in, rest_in, sems):
        row, dp = lax.axis_index("row"), lax.axis_index("dp")
        other = lax.rem(dp + 1, n_dp)
        copies = [
            pltpu.make_async_remote_copy(
                src_ref=src.at[other], dst_ref=dst, send_sem=sems.at[i, 0], recv_sem=sems.at[i, 1],
                device_id={"row": row, "dp": other}, device_id_type=MESH)
            for i, (src, dst) in enumerate(((cand_ref, cand_in), (rest_ref, rest_in)))]
        greet(n_row, n_dp, False, True)
        for c in copies:
            c.start()
        for c in copies:
            c.wait()

        def one(r, carry):
            z, y, x = coords(r, side)
            a, b, c = order(0, z, y, x)
            s0[a, b, c] = cand_ref[dp, r, 0] + cand_in[r, 0]
            a, b, c = order(1, z, y, x)
            s1[a, b, c] = cand_ref[dp, r, 1] + cand_in[r, 1]
            a, b, c = order(2, z, y, x)
            s2[a, b, c] = rest_ref[dp, r] + rest_in[r]
            return carry
        lax.fori_loop(0, n_row, one, 0)

    lead = (side, side, side)
    return pl.pallas_call(
        kernel,
        out_shape=[jax.ShapeDtypeStruct(lead + (n, width), jnp.float32) for n in (rows, rows, rest.shape[2])],
        in_specs=[VMEM, VMEM],
        out_specs=[VMEM] * 3,
        scratch_shapes=[
            pltpu.VMEM(cand.shape[1:], jnp.float32),
            pltpu.VMEM(rest.shape[1:], jnp.float32),
            pltpu.SemaphoreType.DMA((2, 2)),
        ],
        compiler_params=params(0),
    )(cand, rest)


def axis_sum(side, n_dp, parts, moved):
    n_row = side ** 3
    n_p, n_m = len(parts), len(moved)
    f32 = jnp.float32

    def kernel(*refs):
        refs = list(refs)
        take = lambda n: [refs.pop(0) for _ in range(n)]
        s, out = take(n_p), take(n_m)
        g, into = take(n_p), take(n_m)
        r1, t1, r2, t2, r3 = (take(n_p) for _ in range(5))
        sems, m_sems = refs
        row, dp = lax.axis_index("row"), lax.axis_index("dp")
        z, y, x = coords(row, side)
        at = [order(p, z, y, x) for p in range(n_p)]
        greet(n_row, n_dp, True, False)

        def send(p, phase, axis, k, src, dst):
            to = list(at[p])
            to[axis] = lax.rem(to[axis] + k, side)
            pltpu.make_async_remote_copy(
                src_ref=src(to[axis]), dst_ref=dst, send_sem=sems.at[p, phase, 0], recv_sem=sems.at[p, phase, 1],
                device_id={"row": row_of(p, *to, side), "dp": dp}, device_id_type=MESH).start()

        def wait(p, phase, d, like):
            pltpu.make_async_copy(like, like, sems.at[p, phase, d]).wait()

        def move(lo, hi):
            def one(j, carry):
                peer = lax.rem(row + j, n_row)
                for i in range(n_m):
                    pltpu.make_async_remote_copy(
                        src_ref=out[i].at[peer], dst_ref=into[i].at[row], send_sem=m_sems.at[i, 0], recv_sem=m_sems.at[i, 1],
                        device_id={"row": peer, "dp": dp}, device_id_type=MESH).start()
                return carry
            lax.fori_loop(lo, hi, one, 0)
        cuts = [1 + (n_row - 1) * i // 6 for i in range(7)]

        src_of = (s, t1, t2)
        got_of = (r1, r2, r3)
        sum_of = (t1, t2, None)
        for phase in range(3):
            for p in range(n_p):
                for k in range(1, side):
                    send(p, phase, phase, k, lambda i, p=p: src_of[phase][p].at[i], got_of[phase][p].at[at[p][phase]])
            move(cuts[phase], cuts[phase + 1])
            if phase == 0:
                for i in range(n_m):
                    pltpu.make_async_copy(out[i].at[row], into[i].at[row], m_sems.at[i, 1]).start()
            for p in range(n_p):
                mine, got = src_of[phase][p], got_of[phase][p]
                wait(p, phase, 1, got.at[pl.ds(0, side - 1)])
                me = at[p][phase]

                def total(idx, p=p, mine=mine, got=got, me=me):
                    v = mine[(me,) + idx]
                    for k in range(1, side):
                        v = v + got[(lax.rem(me + k, side),) + idx]
                    return v
                if phase == 0:
                    def body(i, carry, p=p, total=total):
                        for j in range(side):
                            t1[p][i, j] = total((i, j))
                        return carry
                    lax.fori_loop(0, side, body, 0)
                elif phase == 1:
                    def body(i, carry, p=p, total=total):
                        t2[p][i] = total((i,))
                        return carry
                    lax.fori_loop(0, side, body, 0)
                else:
                    g[p][at[p][0], at[p][1], at[p][2]] = total(())

        for phase in range(3, 6):
            axis = 5 - phase
            for p in range(n_p):
                blk = g[p].at[at[p][:axis + 1]]
                for k in range(1, side):
                    send(p, phase, axis, k, lambda i, blk=blk: blk, blk)
            move(cuts[phase], cuts[phase + 1])
            for p in range(n_p):
                wait(p, phase, 1, g[p].at[at[p][:axis] + (pl.ds(0, side - 1),)])
        for p in range(n_p):
            for phase in range(3):
                wait(p, phase, 0, src_of[phase][p].at[pl.ds(0, side - 1)])
                axis = 2 - phase
                wait(p, phase + 3, 0, g[p].at[at[p][:axis] + (pl.ds(0, side - 1),)])
        for i in range(n_m):
            sent = out[i].at[pl.ds(0, n_row - 1)]
            pltpu.make_async_copy(sent, sent, m_sems.at[i, 0]).wait()
            pltpu.make_async_copy(into[i], into[i], m_sems.at[i, 1]).wait()

    same = [jax.ShapeDtypeStruct(v.shape, v.dtype) for v in list(parts) + list(moved)]
    scratch = [[pltpu.VMEM(shape(v.shape), f32) for v in parts] for shape in (
        lambda q: q, lambda q: q[1:], lambda q: q[1:], lambda q: q[2:], lambda q: q[2:])]
    return pl.pallas_call(
        kernel,
        out_shape=same,
        in_specs=[VMEM] * len(same),
        out_specs=[VMEM] * len(same),
        scratch_shapes=[v for group in scratch for v in group] + [
            pltpu.SemaphoreType.DMA((n_p, 6, 2)), pltpu.SemaphoreType.DMA((n_m, 2))],
        compiler_params=params(4),
    )(*parts, *moved)


def core_swap(n_dp, *xs):
    n = len(xs)

    def kernel(*refs):
        ins, outs, sems = refs[:n], refs[n:2 * n], refs[2 * n]
        row, dp = lax.axis_index("row"), lax.axis_index("dp")
        other = lax.rem(dp + 1, n_dp)
        copies = []
        for i in range(n):
            copies.append(pltpu.make_async_remote_copy(
                src_ref=ins[i], dst_ref=outs[i].at[dp], send_sem=sems.at[i, 0], recv_sem=sems.at[i, 1],
                device_id={"row": row, "dp": other}, device_id_type=MESH))
            copies.append(pltpu.make_async_copy(ins[i], outs[i].at[dp], sems.at[i, 2]))
        greet(1, n_dp, False, True)
        for c in copies:
            c.start()
        for c in copies:
            c.wait()

    return pl.pallas_call(
        kernel,
        out_shape=[jax.ShapeDtypeStruct((n_dp,) + x.shape, x.dtype) for x in xs],
        in_specs=[VMEM] * n,
        out_specs=[VMEM] * n,
        scratch_shapes=[pltpu.SemaphoreType.DMA((n, 3))],
        compiler_params=params(1),
    )(*xs)


def add_rows(n_rows, groups, grad=None, n_acc=4):
    width = groups[0][2].shape[1]
    n_full = n_rows + 8
    chunk = min(128, n_rows)
    flat, specs = [], []
    for row_ids, counts, vals, extra in groups:
        flat += [row_ids, counts, vals, extra]
        specs += [SMEM, SMEM, VMEM, SMEM]
    if grad is not None:
        flat.append(grad)
        specs.append(ANY)

    def kernel(*refs):
        refs = list(refs)
        work = []
        for _ in groups:
            work.append([refs.pop(0) for _ in range(4)])
        grad_ref = refs.pop(0) if grad is not None else None
        out_ref, wide, sem = refs[0], refs[-2], refs[-1]
        accs = refs[1:-2]
        hid_ref = work[0][2]
        part = hid_ref.shape[0] // (groups[0][0].shape[0] // 2)

        def widen(k, carry):
            sl = pl.ds(pl.multiple_of(k * part, part), part)
            wide[sl, :] = hid_ref[sl, :].astype(jnp.float32)
            return carry
        lax.fori_loop(0, hid_ref.shape[0] // part, widen, 0)
        if grad_ref is not None:
            cp_in = pltpu.make_async_copy(grad_ref, accs[0].at[pl.ds(0, n_rows)], sem)
            cp_in.start()
        fresh = accs if grad_ref is None else accs[1:]

        def clear(k, carry):
            for a in fresh:
                a[pl.ds(pl.multiple_of(k * chunk, chunk), chunk), :] = jnp.zeros((chunk, width), jnp.float32)
            return carry
        if fresh:
            lax.fori_loop(0, n_rows // chunk, clear, 0)
        for a in accs:
            a[pl.ds(n_rows, 8), :] = jnp.zeros((8, width), jnp.float32)
        if grad_ref is not None:
            cp_in.wait()

        for which, (idx, cnt, vals_ref, extra) in enumerate(work):
            per_list = vals_ref.shape[0] // idx.shape[0]

            def one_list(i, carry, which=which, idx=idx, cnt=cnt, vals_ref=vals_ref, extra=extra, per_list=per_list):
                def group(q, c2):
                    for u in range(8):
                        c = q * 8 + u
                        acc = accs[u % n_acc]
                        r = idx[i, c]
                        if which == 0:
                            acc[pl.ds(r, 1), :] += extra[i, c] * wide[pl.ds(i * per_list + c, 1), :]
                        else:
                            acc[pl.ds(r, 1), :] += vals_ref[pl.ds(extra[i, c], 1), :]
                    return c2
                return lax.fori_loop(0, (cnt[i] + 7) // 8, group, carry)
            lax.fori_loop(0, idx.shape[0], one_list, 0)

        if n_acc > 1:
            def merge(k, carry):
                sl = pl.ds(pl.multiple_of(k * chunk, chunk), chunk)
                tot = accs[0][sl, :]
                for a in accs[1:]:
                    tot = tot + a[sl, :]
                accs[0][sl, :] = tot
                return carry
            lax.fori_loop(0, n_rows // chunk, merge, 0)
        cp_out = pltpu.make_async_copy(accs[0].at[pl.ds(0, n_rows)], out_ref, sem)
        cp_out.start()
        cp_out.wait()

    return pl.pallas_call(
        kernel,
        out_shape=jax.ShapeDtypeStruct((n_rows, width), jnp.float32),
        in_specs=specs,
        out_specs=ANY,
        scratch_shapes=[pltpu.VMEM((n_full, width), jnp.float32)] * n_acc + [
            pltpu.VMEM(groups[0][2].shape, jnp.float32), pltpu.SemaphoreType.DMA],
        compiler_params=pltpu.CompilerParams(vmem_limit_bytes=60 * 1024 * 1024),
    )(*flat)


def ranks(owner, n_row):
    n = owner.shape[0]
    hot = (owner[:, None] == jnp.arange(n_row)[None, :]).astype(jnp.bfloat16)
    pos = jnp.arange(n)
    before = (pos[:, None] > pos[None, :]).astype(jnp.bfloat16)
    earlier = jnp.dot(before, hot, preferred_element_type=jnp.float32)
    hot32 = hot.astype(jnp.float32)
    return jnp.sum(earlier * hot32, axis=1).astype(jnp.int32), jnp.sum(hot32, axis=0).astype(jnp.int32)


def to_slots(slot, vals, n_slots):
    hit = slot[:, None] == jnp.arange(n_slots)[None, :]
    return [jnp.sum(jnp.where(hit, v[:, None], jnp.zeros((), v.dtype)), axis=0) for v in vals]


def tile_rows(rows, n_row):
    padded = [jnp.pad(r, ((0, 0), (0, LANES - r.shape[1]))) for r in rows]
    padded += [jnp.zeros_like(padded[0])] * (8 - len(rows))
    return jnp.stack(padded, axis=1)


def solution(mesh):
    n_row, n_dp = mesh.shape["row"], mesh.shape["dp"]
    n_dev = n_row * n_dp
    side = round(n_row ** (1 / 3))

    def run_step(x_tok, w_up, w_down, item_table, cand_ids, log_q, targets):
        n_total = x_tok.shape[0]

        def device_step(x_loc, w_up, w_down, tab_loc, cand_ids, log_q, y_loc):
            rows_local, width = tab_loc.shape
            n_tok = y_loc.shape[0]
            n_cand = cand_ids.shape[0]
            row, dp = lax.axis_index("row"), lax.axis_index("dp")
            me = dp * n_row + row
            chunk = n_cand // n_dev
            f32, bf16 = jnp.float32, jnp.bfloat16
            n_ids = n_tok + chunk
            n_pad = -(-n_ids // LANES) * LANES

            my_cands = lax.dynamic_slice_in_dim(cand_ids, me * chunk, chunk)
            ids = jnp.concatenate([y_loc, my_cands])
            owner, local = ids // rows_local, ids % rows_local
            rank, per_owner = ranks(owner, n_row)
            most = jnp.max(per_owner)

            pre_act = jnp.dot(x_loc, w_up, preferred_element_type=f32)
            act_full, gelu_vjp = jax.vjp(jax.nn.gelu, pre_act)
            act_b = act_full.astype(bf16)
            hidden = jnp.dot(act_b, w_down, preferred_element_type=f32).astype(bf16)

            split = jnp.pad(jnp.stack([local // 128, local % 128], axis=1).astype(bf16), ((0, n_pad - n_ids), (0, LANES - 2)))
            carried = jnp.concatenate([jnp.pad(hidden, ((0, n_pad - n_tok), (0, 0))), split], axis=1)

            def pack_round(k):
                rel = rank - k * CAP
                hit = (rel >= 0) & (rel < CAP)
                slot = jnp.where(hit, owner * LANES + rel, -1)
                hid_out, want = pack(jnp.pad(slot, (0, n_pad - n_ids), constant_values=-1)[None, :], carried, n_row)
                return hit, owner * CAP + rel, hid_out, want

            def fetch_round(k):
                hit, at, hid_out, want = pack_round(k)
                lane = jnp.arange(LANES)[None, None, :]
                rows_in, most_all = fetch(n_row, n_dp, jnp.where(lane == LANES - 1, most, want), tab_loc)
                got = jnp.take(rows_in.reshape(n_row * CAP, width), at, axis=0, mode="clip")
                return hit, got, hid_out, want, most_all

            _, got, hid_out, want, most_dp = fetch_round(0)
            cand_rows, most_all = gather_cands(n_row, n_dp, got, n_tok, most_dp)
            most_all = most_all[0, LANES - 1]

            def fetch_more(carry):
                k, got, _ = carry
                hit, new, _, _, most = fetch_round(k)
                got = jnp.where(hit[:, None], new, got)
                return k + 1, got, gather_cands(n_row, n_dp, got, n_tok, most)[0]

            _, got, cand_rows = lax.while_loop(
                lambda c: c[0] * CAP < most_all, fetch_more, (jnp.int32(1), got, cand_rows))
            cand_rows = cand_rows.reshape(n_cand, width)

            cand_grad, grad_hid, dz_lanes, loss_part = softmax(
                n_total, cand_rows, hidden, got,
                jnp.broadcast_to(y_loc[:, None], (n_tok, LANES)), cand_ids[None, :], log_q[None, :])
            dz_tgt, loss_sum = dz_lanes[:, 0], loss_part[0, 0]

            grad_down = jnp.einsum("tf,td->fd", act_b, grad_hid, preferred_element_type=f32)
            grad_act = jnp.einsum("td,fd->tf", grad_hid, w_down, preferred_element_type=f32)
            grad_pre = gelu_vjp(grad_act)[0].astype(bf16)
            grad_up = jnp.einsum("ti,tf->if", x_loc, grad_pre, preferred_element_type=f32)

            t_rank, t_owner = rank[:n_tok], owner[:n_tok]
            t_count = jnp.sum((t_owner[:, None] == jnp.arange(n_row)[None, :]).astype(jnp.int32), axis=0)
            c_rank, _ = ranks(owner[n_tok:], n_row)
            c_slot = owner[n_tok:] * chunk + c_rank
            c_count = per_owner - t_count
            c_row, c_pos = to_slots(c_slot, [(local[n_tok:] - rows_local).astype(f32), jnp.arange(chunk, dtype=f32)], n_row * chunk)
            c_row = (c_row + rows_local).reshape(n_row, chunk)
            c_pos = c_pos.reshape(n_row, chunk)
            half, z_y_x = chunk // 2, coords(row, side)
            first = []
            for part in range(2):
                a, b, c = order(part, *z_y_x)
                first.append((((part * n_dp + dp) * n_row + (a * side + b) * side + c) * half).astype(f32))
            c_pos = jnp.where(c_pos < half, first[0] + c_pos, first[1] + c_pos - half)

            def give(k, want):
                rel = t_rank - k * CAP
                slot = jnp.where((rel >= 0) & (rel < CAP), t_owner * CAP + rel, -1)
                (t_dz,) = to_slots(slot, [dz_tgt], n_row * CAP)
                t_row = want[:, 0, :CAP].astype(f32)
                now = jnp.clip(t_count - k * CAP, 0, CAP).astype(f32)
                counts = jnp.stack([now, c_count.astype(f32), jnp.full((n_row,), loss_sum)], axis=1)
                return tile_rows([t_row.reshape(n_row, CAP), t_dz.reshape(n_row, CAP), c_row, c_pos, counts], n_row)

            to_int = lambda v: v.astype(jnp.int32)

            def token_group(hid_in, meta_in):
                return to_int(meta_in[:, 0, :CAP]), to_int(meta_in[:, 4, 0]), hid_in.reshape(n_dev * CAP, width), meta_in[:, 1, :CAP]

            blocks = w_up.shape[1] // LANES
            up_shape = (n_dev // blocks, w_up.shape[0] * blocks // n_dev, blocks, LANES)
            rest = jnp.concatenate([
                grad_up.reshape(up_shape).transpose(0, 2, 1, 3).reshape(n_dp, n_row, up_shape[1], width),
                grad_down.reshape(n_dp, n_row, -1, width)], axis=2)
            parts = core_sum(side, cand_grad.reshape(n_dp, n_row, 2, half, width), rest)
            g0, g1, g2, hid_in, meta_in = axis_sum(side, n_dp, parts, [hid_out, give(0, want)])
            g0, g1, g2, hid_in, meta_in = core_swap(n_dp, g0, g1, g2, hid_in, meta_in)
            hid_in, meta_in = hid_in.reshape(n_dev, CAP, width), meta_in.reshape(n_dev, 8, LANES)
            cand_sums = jnp.concatenate([g0.reshape(-1, width), g1.reshape(-1, width)], axis=0)
            rest = jnp.transpose(g2, (0, 1, 3, 2, 4, 5)).reshape(n_dev, -1, width)
            grad_up = rest[:, :up_shape[1]].reshape(up_shape[0], blocks, up_shape[1], LANES).transpose(0, 2, 1, 3).reshape(w_up.shape)
            grad_down = rest[:, up_shape[1]:].reshape(w_down.shape)

            grad = add_rows(rows_local, [
                token_group(hid_in, meta_in),
                (to_int(meta_in[:, 2, :chunk]), to_int(meta_in[:, 4, 1]), cand_sums, to_int(meta_in[:, 3, :chunk]))])

            def give_more(carry):
                k, grad = carry
                _, _, hid_more, want_more = pack_round(k)
                return k + 1, add_rows(rows_local, [token_group(*exchange(n_row, n_dp, True, hid_more, give(k, want_more)))], grad, 1)

            _, grad = lax.while_loop(lambda c: c[0] * CAP < most_all, give_more, (jnp.int32(1), grad))
            return jnp.sum(meta_in[:, 4, 2]) / n_total, grad, grad_up, grad_down

        return jax.shard_map(
            device_step,
            mesh=mesh,
            in_specs=(P(ALL_AXES, None), P(), P(), P("row", None), P(), P(), P(ALL_AXES)),
            out_specs=(P(), P("row", None), P(), P()),
            check_vma=False,
        )(x_tok, w_up, w_down, item_table, cand_ids, log_q, targets)

    return run_step
```

```python
import functools

import jax
import jax.numpy as jnp
from jax import lax
from jax.experimental import pallas as pl
from jax.experimental.pallas import tpu as pltpu
from jax.sharding import PartitionSpec as P

ALL_AXES = ("dp", "row")
MESH = pl.DeviceIdType.MESH
CAP = 112
BLK = 2048
TOK = 256
LANES = 128
ANY = pl.BlockSpec(memory_space=pl.ANY)
VMEM = pl.BlockSpec(memory_space=pltpu.VMEM)
SMEM = pl.BlockSpec(memory_space=pltpu.SMEM)


def params(barrier=None):
    return pltpu.CompilerParams(has_side_effects=True, vmem_limit_bytes=60 * 1024 * 1024, collective_id=barrier)


def greet(n_row, n_dp, rows, partner):
    row, dp = lax.axis_index("row"), lax.axis_index("dp")
    barrier = pltpu.get_barrier_semaphore()
    if partner:
        pl.semaphore_signal(barrier, inc=1, device_id={"row": row, "dp": lax.rem(dp + 1, n_dp)}, device_id_type=MESH)
    if rows:
        def one(j, carry):
            pl.semaphore_signal(barrier, inc=1, device_id={"row": lax.rem(row + j, n_row), "dp": dp}, device_id_type=MESH)
            return carry
        lax.fori_loop(1, n_row, one, 0)
    pl.semaphore_wait(barrier, (n_row - 1 if rows else 0) + (1 if partner else 0))


def exchange(n_row, n_dp, both, *xs):
    n_x = len(xs)
    steps = range(n_dp) if both else range(1)
    n_out = n_row * (n_dp if both else 1)

    def kernel(*refs):
        ins, outs = refs[:n_x], refs[n_x:2 * n_x]
        send_sem, recv_sem = refs[2 * n_x:]
        row, dp = lax.axis_index("row"), lax.axis_index("dp")
        slot = dp * n_row + row if both else row
        for i in range(n_x):
            pltpu.make_async_copy(ins[i].at[row], outs[i].at[slot], recv_sem.at[i]).start()

        for e in steps:
            def send(j, carry, e=e):
                peer = lax.rem(row + j, n_row)
                for i in range(n_x):
                    pltpu.make_async_remote_copy(
                        src_ref=ins[i].at[peer],
                        dst_ref=outs[i].at[slot],
                        send_sem=send_sem.at[i, e],
                        recv_sem=recv_sem.at[i],
                        device_id={"row": peer, "dp": lax.rem(dp + e, n_dp)},
                        device_id_type=MESH,
                    ).start()
                return carry
            lax.fori_loop(0 if e else 1, n_row, send, 0)
        for i in range(n_x):
            for e in steps:
                sent = ins[i] if e else ins[i].at[pl.ds(0, n_row - 1)]
                pltpu.make_async_copy(sent, sent, send_sem.at[i, e]).wait()
            pltpu.make_async_copy(outs[i], outs[i], recv_sem.at[i]).wait()

    return pl.pallas_call(
        kernel,
        out_shape=[jax.ShapeDtypeStruct((n_out,) + x.shape[1:], x.dtype) for x in xs],
        in_specs=[VMEM] * n_x,
        out_specs=[VMEM] * n_x,
        scratch_shapes=[pltpu.SemaphoreType.DMA((n_x, n_dp)), pltpu.SemaphoreType.DMA((n_x,))],
        compiler_params=params(),
    )(*xs)


def pack(slot_row, vals, n_row):
    n_pad = slot_row.shape[1]
    per = 4 if n_row % 4 == 0 else 1

    def kernel(slot_ref, vals_ref, hid_ref, want_ref):
        base = pl.program_id(0) * (per * LANES)
        at = lax.broadcasted_iota(jnp.int32, (per * LANES, n_pad), 0) + base
        hit = (at == slot_ref[...]).astype(jnp.float32).astype(jnp.bfloat16)
        got = jnp.dot(hit, vals_ref[...], preferred_element_type=jnp.float32)
        for o in range(per):
            blk = got[o * LANES:(o + 1) * LANES]
            hid_ref[o] = blk[:CAP, :LANES].astype(jnp.bfloat16)
            ids = jnp.transpose(blk[:, LANES:])
            want_ref[o] = (ids[0:1] * 128.0 + ids[1:2]).astype(jnp.int32)

    return pl.pallas_call(
        kernel,
        grid=(n_row // per,),
        out_shape=[
            jax.ShapeDtypeStruct((n_row, CAP, LANES), jnp.bfloat16),
            jax.ShapeDtypeStruct((n_row, 1, LANES), jnp.int32),
        ],
        in_specs=[pl.BlockSpec((1, n_pad), lambda i: (0, 0)), pl.BlockSpec((n_pad, 2 * LANES), lambda i: (0, 0))],
        out_specs=[
            pl.BlockSpec((per, CAP, LANES), lambda i: (i, 0, 0)),
            pl.BlockSpec((per, 1, LANES), lambda i: (i, 0, 0)),
        ],
        compiler_params=pltpu.CompilerParams(vmem_limit_bytes=40 * 1024 * 1024),
    )(slot_row, vals)


def place(base, slot_lanes, dz_lanes):
    n_row, n_tok = base.shape[0], dz_lanes.shape[0]
    per, step = 4, 64

    def kernel(base_ref, slot_ref, dz_ref, out_ref):
        first = pl.program_id(0) * per
        lane = lax.broadcasted_iota(jnp.int32, (step, LANES), 1)

        def some(k, sums):
            sl = pl.ds(pl.multiple_of(k * step, step), step)
            slot, dz = slot_ref[sl, :] - first * LANES - lane, dz_ref[sl, :]
            picked = [jnp.where(slot == o * LANES, dz, 0.0).reshape(step // 8, 8, LANES) for o in range(per)]
            return tuple(s + jnp.sum(v, axis=0) for s, v in zip(sums, picked))
        sums = lax.fori_loop(0, n_tok // step, some, (jnp.zeros((8, LANES), jnp.float32),) * per)
        which = lax.broadcasted_iota(jnp.int32, (8, LANES), 0)
        for o in range(per):
            out_ref[o] = base_ref[o] + jnp.where(which == 1, jnp.sum(sums[o], axis=0, keepdims=True), 0.0)

    tile = pl.BlockSpec((per, 8, LANES), lambda i: (i, 0, 0))
    whole = pl.BlockSpec((n_tok, LANES), lambda i: (0, 0))
    return pl.pallas_call(
        kernel,
        grid=(n_row // per,),
        out_shape=jax.ShapeDtypeStruct(base.shape, base.dtype),
        in_specs=[tile, whole, whole],
        out_specs=tile,
        compiler_params=pltpu.CompilerParams(vmem_limit_bytes=40 * 1024 * 1024),
    )(base, slot_lanes, dz_lanes)


def fetch(n_row, n_dp, want, table):
    rows_local, width = table.shape
    cut = min(1024, rows_local // 2)
    n_cut = rows_local // cut

    def kernel(want_ref, tab_ref, rows_ref, most_ref, tab16, tab32, asked, ask_s, stage, out_buf, sems, tab_sem):
        row, dp = lax.axis_index("row"), lax.axis_index("dp")

        def load(k, p):
            sl = pl.ds(pl.multiple_of(k * cut, cut), cut)
            return pltpu.make_async_copy(tab_ref.at[sl], tab16.at[p], tab_sem.at[p])
        load(0, 0).start()
        load(1, 1).start()
        greet(n_row, n_dp, True, False)
        pltpu.make_async_copy(want_ref.at[row], asked.at[row], sems.at[1]).start()

        def ask(j, carry):
            peer = lax.rem(row + j, n_row)
            pltpu.make_async_remote_copy(
                src_ref=want_ref.at[peer], dst_ref=asked.at[row], send_sem=sems.at[0], recv_sem=sems.at[1],
                device_id={"row": peer, "dp": dp}, device_id_type=MESH).start()
            return carry
        lax.fori_loop(1, n_row, ask, 0)

        def widen(k, more):
            for p in range(2):
                load(2 * k + p, p).wait()
                sl = pl.ds(pl.multiple_of((2 * k + p) * cut, cut), cut)
                tab32[sl, :] = tab16[p].astype(jnp.float32)
                if more:
                    load(2 * k + p + 2, p).start()
            return 0
        lax.fori_loop(0, n_cut // 2 - 1, lambda k, c: widen(k, True), 0)
        widen(n_cut // 2 - 1, False)
        pltpu.make_async_copy(asked, asked, sems.at[1]).wait()
        to_s = pltpu.make_async_copy(asked, ask_s, tab_sem.at[0])
        to_s.start()
        most_ref[...] = jnp.broadcast_to(jnp.max(asked[...], axis=0), (8, LANES))
        to_s.wait()

        def send(peer):
            pltpu.make_async_remote_copy(
                src_ref=out_buf.at[peer], dst_ref=rows_ref.at[row], send_sem=sems.at[2], recv_sem=sems.at[3],
                device_id={"row": peer, "dp": dp}, device_id_type=MESH).start()

        def gather(j):
            peer = lax.rem(row + j, n_row)
            for c in range(CAP):
                stage[pl.ds(c, 1), :] = tab32[pl.ds(ask_s[peer, 0, c], 1), :]
            out_buf[peer] = stage[...].astype(jnp.bfloat16)

        def step(j, carry):
            gather(j)

            @pl.when(j > 1)
            def _():
                send(lax.rem(row + j - 1, n_row))
            return carry
        lax.fori_loop(1, n_row + 1, step, 0)
        pltpu.make_async_copy(out_buf.at[row], rows_ref.at[row], sems.at[3]).start()
        sent = want_ref.at[pl.ds(0, n_row - 1)]
        pltpu.make_async_copy(sent, sent, sems.at[0]).wait()
        sent = out_buf.at[pl.ds(0, n_row - 1)]
        pltpu.make_async_copy(sent, sent, sems.at[2]).wait()
        pltpu.make_async_copy(rows_ref, rows_ref, sems.at[3]).wait()

    return pl.pallas_call(
        kernel,
        out_shape=[
            jax.ShapeDtypeStruct((n_row, CAP, width), table.dtype),
            jax.ShapeDtypeStruct((8, LANES), jnp.int32),
        ],
        in_specs=[VMEM, ANY],
        out_specs=[VMEM, VMEM],
        scratch_shapes=[
            pltpu.VMEM((2, cut, width), table.dtype),
            pltpu.VMEM((rows_local, width), jnp.float32),
            pltpu.VMEM((n_row, 1, LANES), jnp.int32),
            pltpu.SMEM((n_row, 1, LANES), jnp.int32),
            pltpu.VMEM((CAP, width), jnp.float32),
            pltpu.VMEM((n_row, CAP, width), table.dtype),
            pltpu.SemaphoreType.DMA((4,)),
            pltpu.SemaphoreType.DMA((2,)),
        ],
        compiler_params=params(2),
    )(want, table)


def gather_cands(n_row, n_dp, got, n_tok, most):
    chunk, width = got.shape[0] - n_tok, got.shape[1]

    def kernel(got_ref, most_ref, all_ref, top_ref, theirs, sems):
        mine_ref = got_ref.at[pl.ds(n_tok, chunk)]
        row, dp = lax.axis_index("row"), lax.axis_index("dp")
        other = lax.rem(dp + 1, n_dp)
        me = dp * n_row + row

        greet(n_row, n_dp, True, True)

        def one(j, carry):
            peer = lax.rem(row + j, n_row)
            pltpu.make_async_remote_copy(
                src_ref=mine_ref, dst_ref=all_ref.at[me], send_sem=sems.at[0], recv_sem=sems.at[1],
                device_id={"row": peer, "dp": dp}, device_id_type=MESH).start()
            return carry
        lax.fori_loop(1, n_row, one, 0)
        pltpu.make_async_copy(mine_ref, all_ref.at[me], sems.at[1]).start()
        count = pltpu.make_async_remote_copy(
            src_ref=most_ref, dst_ref=theirs, send_sem=sems.at[4], recv_sem=sems.at[5],
            device_id={"row": row, "dp": other}, device_id_type=MESH)
        count.start()
        half = all_ref.at[pl.ds(dp * n_row, n_row)]
        pltpu.make_async_copy(half, half, sems.at[1]).wait()
        swap = pltpu.make_async_remote_copy(
            src_ref=half, dst_ref=half, send_sem=sems.at[2], recv_sem=sems.at[3],
            device_id={"row": row, "dp": other}, device_id_type=MESH)
        swap.start()
        count.wait()
        top_ref[...] = jnp.maximum(most_ref[...], theirs[...])
        sent = all_ref.at[pl.ds(0, n_row - 1)]
        pltpu.make_async_copy(sent, sent, sems.at[0]).wait()
        swap.wait()

    return pl.pallas_call(
        kernel,
        out_shape=[
            jax.ShapeDtypeStruct((n_dp * n_row, chunk, width), got.dtype),
            jax.ShapeDtypeStruct(most.shape, most.dtype),
        ],
        in_specs=[VMEM, VMEM],
        out_specs=[VMEM, VMEM],
        scratch_shapes=[pltpu.VMEM(most.shape, most.dtype), pltpu.SemaphoreType.DMA((6,))],
        compiler_params=params(3),
    )(got, most)


def softmax(n_total, cand_rows, hidden, tgt, y_lanes, cand_ids, log_q):
    n_cand, width = cand_rows.shape
    n_tok = hidden.shape[0]
    n_blk, n_sub = n_cand // BLK, n_tok // TOK
    f32 = jnp.float32

    def kernel(cands, h_ref, t_ref, y_ref, id_ref, lq_ref, cg_ref, dh_ref, dz_ref, loss_ref, z, g, h_t, acc, stat):
        h_t[...] = jnp.transpose(h_ref[...].astype(f32)).astype(jnp.bfloat16)
        for s in range(n_sub):
            tok = pl.ds(s * TOK, TOK)
            prod = h_ref[tok, :].astype(f32) * t_ref[tok, :].astype(f32)
            z_tgt = jnp.broadcast_to(jnp.sum(prod, axis=1, keepdims=True), (TOK, LANES))
            stat[0, tok, :] = z_tgt
            stat[1, tok, :] = z_tgt
        def logits(b, carry):
            rows = cands[pl.ds(pl.multiple_of(b * BLK, BLK), BLK), :]
            cols = pl.ds(pl.multiple_of(b * BLK, BLK), BLK)
            lq, cid = lq_ref[:, cols], id_ref[:, cols]

            def sub(s, c2):
                tok = pl.ds(pl.multiple_of(s * TOK, TOK), TOK)
                zz = lax.dot_general(h_ref[tok, :], rows, (((1,), (1,)), ((), ())), preferred_element_type=f32) - lq
                y = y_ref[tok, :]
                top = stat[1, tok, :]
                for k in range(BLK // LANES):
                    ln = slice(k * LANES, (k + 1) * LANES)
                    part = jnp.where(y == cid[:, ln], -1e9, zz[:, ln])
                    z[tok, pl.ds(pl.multiple_of(b * BLK + k * LANES, LANES), LANES)] = part
                    top = jnp.maximum(top, part)
                stat[1, tok, :] = top
                return c2
            return lax.fori_loop(0, n_sub, sub, carry)
        lax.fori_loop(0, n_blk, logits, 0)

        for s in range(n_sub):
            tok = pl.ds(s * TOK, TOK)
            stat[1, tok, :] = jnp.broadcast_to(jnp.max(stat[1, tok, :], axis=1, keepdims=True), (TOK, LANES))
            stat[2, tok, :] = jnp.zeros((TOK, LANES), f32)

        def exps(b, carry):
            def sub(s, c2):
                tok = pl.ds(pl.multiple_of(s * TOK, TOK), TOK)
                top = stat[1, tok, :]
                tot = stat[2, tok, :]
                for k in range(BLK // LANES):
                    at = pl.ds(pl.multiple_of(b * BLK + k * LANES, LANES), LANES)
                    e = jnp.exp(z[tok, at] - top)
                    z[tok, at] = e
                    tot = tot + e
                stat[2, tok, :] = tot
                return c2
            return lax.fori_loop(0, n_sub, sub, carry)
        lax.fori_loop(0, n_blk, exps, 0)

        loss_ref[...] = jnp.zeros_like(loss_ref)
        for s in range(n_sub):
            tok = pl.ds(s * TOK, TOK)
            z_tgt, top = stat[0, tok, :], stat[1, tok, :]
            e_tgt = jnp.exp(z_tgt - top)
            total = e_tgt + jnp.broadcast_to(jnp.sum(stat[2, tok, :], axis=1, keepdims=True), (TOK, LANES))
            dz = (e_tgt / total - 1.0) * (1.0 / n_total)
            dz_ref[tok, :] = dz
            stat[2, tok, :] = (1.0 / total) * (1.0 / n_total)
            part = top + jnp.log(total) - z_tgt
            loss_ref[...] += jnp.broadcast_to(jnp.sum(part, axis=0, keepdims=True), loss_ref.shape)
            acc[tok, :] = dz * t_ref[tok, :].astype(f32)

        def grads(b, carry):
            rows = cands[pl.ds(pl.multiple_of(b * BLK, BLK), BLK), :]

            def sub(s, c2):
                tok = pl.ds(pl.multiple_of(s * TOK, TOK), TOK)
                inv = stat[2, tok, :]
                for k in range(BLK // LANES):
                    at = pl.ds(pl.multiple_of(b * BLK + k * LANES, LANES), LANES)
                    g[tok, k * LANES:(k + 1) * LANES] = (z[tok, at] * inv).astype(jnp.bfloat16)
                acc[tok, :] += jnp.dot(g[tok, :], rows, preferred_element_type=f32)
                return c2
            lax.fori_loop(0, n_sub, sub, 0)
            cg_t = jnp.dot(h_t[...], g[...], preferred_element_type=f32)
            cg_ref[pl.ds(pl.multiple_of(b * BLK, BLK), BLK), :] = jnp.transpose(cg_t)
            return carry
        lax.fori_loop(0, n_blk, grads, 0)
        dh_ref[...] = acc[...].astype(jnp.bfloat16)

    return pl.pallas_call(
        kernel,
        out_shape=[
            jax.ShapeDtypeStruct((n_cand, width), f32),
            jax.ShapeDtypeStruct((n_tok, width), jnp.bfloat16),
            jax.ShapeDtypeStruct((n_tok, LANES), f32),
            jax.ShapeDtypeStruct((8, LANES), f32),
        ],
        in_specs=[VMEM] * 6,
        out_specs=[VMEM] * 4,
        scratch_shapes=[
            pltpu.VMEM((n_tok, n_cand), f32),
            pltpu.VMEM((n_tok, BLK), jnp.bfloat16),
            pltpu.VMEM((width, n_tok), jnp.bfloat16),
            pltpu.VMEM((n_tok, width), f32),
            pltpu.VMEM((3, n_tok, LANES), f32),
        ],
        compiler_params=pltpu.CompilerParams(vmem_limit_bytes=60 * 1024 * 1024),
    )(cand_rows, hidden, tgt, y_lanes, cand_ids, log_q)


def coords(row, side):
    return row // (side * side), lax.rem(row // side, side), lax.rem(row, side)


def order(part, z, y, x):
    return ((x, y, z), (y, z, x), (z, x, y))[part]


def row_of(part, a, b, c, side):
    z, y, x = ((c, b, a), (b, a, c), (a, c, b))[part]
    return (z * side + y) * side + x


def core_sum(side, cand, rest):
    n_row = side ** 3
    n_dp, rows = cand.shape[0], cand.shape[3]
    width = cand.shape[-1]

    def kernel(cand_ref, rest_ref, s0, s1, s2, cand_in, rest_in, sems):
        row, dp = lax.axis_index("row"), lax.axis_index("dp")
        other = lax.rem(dp + 1, n_dp)
        copies = [
            pltpu.make_async_remote_copy(
                src_ref=src.at[other], dst_ref=dst, send_sem=sems.at[i, 0], recv_sem=sems.at[i, 1],
                device_id={"row": row, "dp": other}, device_id_type=MESH)
            for i, (src, dst) in enumerate(((cand_ref, cand_in), (rest_ref, rest_in)))]
        greet(n_row, n_dp, False, True)
        for c in copies:
            c.start()
        for c in copies:
            c.wait()

        def one(r, carry):
            z, y, x = coords(r, side)
            a, b, c = order(0, z, y, x)
            s0[a, b, c] = cand_ref[dp, r, 0] + cand_in[r, 0]
            a, b, c = order(1, z, y, x)
            s1[a, b, c] = cand_ref[dp, r, 1] + cand_in[r, 1]
            a, b, c = order(2, z, y, x)
            s2[a, b, c] = rest_ref[dp, r] + rest_in[r]
            return carry
        lax.fori_loop(0, n_row, one, 0)

    lead = (side, side, side)
    return pl.pallas_call(
        kernel,
        out_shape=[jax.ShapeDtypeStruct(lead + (n, width), jnp.float32) for n in (rows, rows, rest.shape[2])],
        in_specs=[VMEM, VMEM],
        out_specs=[VMEM] * 3,
        scratch_shapes=[
            pltpu.VMEM(cand.shape[1:], jnp.float32),
            pltpu.VMEM(rest.shape[1:], jnp.float32),
            pltpu.SemaphoreType.DMA((2, 2)),
        ],
        compiler_params=params(0),
    )(cand, rest)


def axis_sum(side, n_dp, parts, moved):
    n_row = side ** 3
    n_p, n_m = len(parts), len(moved)
    f32 = jnp.float32

    def kernel(*refs):
        refs = list(refs)
        take = lambda n: [refs.pop(0) for _ in range(n)]
        s, out = take(n_p), take(n_m)
        g, into = take(n_p), take(n_m)
        r1, t1, r2, t2, r3 = (take(n_p) for _ in range(5))
        sems, m_sems = refs
        row, dp = lax.axis_index("row"), lax.axis_index("dp")
        z, y, x = coords(row, side)
        at = [order(p, z, y, x) for p in range(n_p)]
        greet(n_row, n_dp, True, False)

        def send(p, phase, axis, k, src, dst):
            to = list(at[p])
            to[axis] = lax.rem(to[axis] + k, side)
            pltpu.make_async_remote_copy(
                src_ref=src(to[axis]), dst_ref=dst, send_sem=sems.at[p, phase, 0], recv_sem=sems.at[p, phase, 1],
                device_id={"row": row_of(p, *to, side), "dp": dp}, device_id_type=MESH).start()

        def wait(p, phase, d, like):
            pltpu.make_async_copy(like, like, sems.at[p, phase, d]).wait()

        def move(lo, hi):
            def one(j, carry):
                peer = lax.rem(row + j, n_row)
                for i in range(n_m):
                    pltpu.make_async_remote_copy(
                        src_ref=out[i].at[peer], dst_ref=into[i].at[row], send_sem=m_sems.at[i, 0], recv_sem=m_sems.at[i, 1],
                        device_id={"row": peer, "dp": dp}, device_id_type=MESH).start()
                return carry
            lax.fori_loop(lo, hi, one, 0)
        cuts = [1 + (n_row - 1) * i // 6 for i in range(7)]

        src_of = (s, t1, t2)
        got_of = (r1, r2, r3)
        sum_of = (t1, t2, None)
        for phase in range(3):
            for p in range(n_p):
                for k in range(1, side):
                    send(p, phase, phase, k, lambda i, p=p: src_of[phase][p].at[i], got_of[phase][p].at[at[p][phase]])
            move(cuts[phase], cuts[phase + 1])
            if phase == 0:
                for i in range(n_m):
                    pltpu.make_async_copy(out[i].at[row], into[i].at[row], m_sems.at[i, 1]).start()
            for p in range(n_p):
                mine, got = src_of[phase][p], got_of[phase][p]
                wait(p, phase, 1, got.at[pl.ds(0, side - 1)])
                me = at[p][phase]

                def total(idx, p=p, mine=mine, got=got, me=me):
                    v = mine[(me,) + idx]
                    for k in range(1, side):
                        v = v + got[(lax.rem(me + k, side),) + idx]
                    return v
                if phase == 0:
                    def body(i, carry, p=p, total=total):
                        for j in range(side):
                            t1[p][i, j] = total((i, j))
                        return carry
                    lax.fori_loop(0, side, body, 0)
                elif phase == 1:
                    def body(i, carry, p=p, total=total):
                        t2[p][i] = total((i,))
                        return carry
                    lax.fori_loop(0, side, body, 0)
                else:
                    g[p][at[p][0], at[p][1], at[p][2]] = total(())

        for phase in range(3, 6):
            axis = 5 - phase
            for p in range(n_p):
                blk = g[p].at[at[p][:axis + 1]]
                for k in range(1, side):
                    send(p, phase, axis, k, lambda i, blk=blk: blk, blk)
            move(cuts[phase], cuts[phase + 1])
            for p in range(n_p):
                wait(p, phase, 1, g[p].at[at[p][:axis] + (pl.ds(0, side - 1),)])
        for p in range(n_p):
            for phase in range(3):
                wait(p, phase, 0, src_of[phase][p].at[pl.ds(0, side - 1)])
                axis = 2 - phase
                wait(p, phase + 3, 0, g[p].at[at[p][:axis] + (pl.ds(0, side - 1),)])
        for i in range(n_m):
            sent = out[i].at[pl.ds(0, n_row - 1)]
            pltpu.make_async_copy(sent, sent, m_sems.at[i, 0]).wait()
            pltpu.make_async_copy(into[i], into[i], m_sems.at[i, 1]).wait()

    same = [jax.ShapeDtypeStruct(v.shape, v.dtype) for v in list(parts) + list(moved)]
    scratch = [[pltpu.VMEM(shape(v.shape), f32) for v in parts] for shape in (
        lambda q: q, lambda q: q[1:], lambda q: q[1:], lambda q: q[2:], lambda q: q[2:])]
    return pl.pallas_call(
        kernel,
        out_shape=same,
        in_specs=[VMEM] * len(same),
        out_specs=[VMEM] * len(same),
        scratch_shapes=[v for group in scratch for v in group] + [
            pltpu.SemaphoreType.DMA((n_p, 6, 2)), pltpu.SemaphoreType.DMA((n_m, 2))],
        compiler_params=params(4),
    )(*parts, *moved)


def core_swap(n_dp, *groups):
    flat = [x for group in groups for x in group]
    n, n_out = len(flat), len(groups)
    where = [(o, p) for o, group in enumerate(groups) for p in range(len(group))]

    def kernel(*refs):
        ins, outs, sems = refs[:n], refs[n:n + n_out], refs[n + n_out]
        row, dp = lax.axis_index("row"), lax.axis_index("dp")
        other = lax.rem(dp + 1, n_dp)
        copies = []
        for i, (o, p) in enumerate(where):
            copies.append(pltpu.make_async_remote_copy(
                src_ref=ins[i], dst_ref=outs[o].at[p, dp], send_sem=sems.at[i, 0], recv_sem=sems.at[i, 1],
                device_id={"row": row, "dp": other}, device_id_type=MESH))
            copies.append(pltpu.make_async_copy(ins[i], outs[o].at[p, dp], sems.at[i, 2]))
        greet(1, n_dp, False, True)
        for c in copies:
            c.start()
        for c in copies:
            c.wait()

    return pl.pallas_call(
        kernel,
        out_shape=[jax.ShapeDtypeStruct((len(g), n_dp) + g[0].shape, g[0].dtype) for g in groups],
        in_specs=[VMEM] * n,
        out_specs=[VMEM] * n_out,
        scratch_shapes=[pltpu.SemaphoreType.DMA((n, 3))],
        compiler_params=params(1),
    )(*flat)


def add_rows(n_rows, groups, grad=None, n_acc=4):
    width = groups[0][2].shape[1]
    n_full = n_rows + 8
    chunk = min(128, n_rows)
    cut = min(128, n_rows // 8)
    flat, specs = [], []
    for row_ids, counts, vals, extra in groups:
        flat += [row_ids, counts, vals, extra]
        specs += [SMEM, SMEM, VMEM, SMEM]
    if grad is not None:
        flat.append(grad)
        specs.append(ANY)

    def kernel(*refs):
        refs = list(refs)
        work = []
        for _ in groups:
            work.append([refs.pop(0) for _ in range(4)])
        grad_ref = refs.pop(0) if grad is not None else None
        out_ref, wide, sem, out_sem = refs[0], refs[-3], refs[-2], refs[-1]
        accs = refs[1:-3]
        hid_ref = work[0][2]
        part = hid_ref.shape[0] // (groups[0][0].shape[0] // 2)

        def widen(k, carry):
            sl = pl.ds(pl.multiple_of(k * part, part), part)
            wide[sl, :] = hid_ref[sl, :].astype(jnp.float32)
            return carry
        lax.fori_loop(0, hid_ref.shape[0] // part, widen, 0)
        if grad_ref is not None:
            cp_in = pltpu.make_async_copy(grad_ref, accs[0].at[pl.ds(0, n_rows)], sem)
            cp_in.start()
        fresh = accs if grad_ref is None else accs[1:]

        def clear(k, carry):
            for a in fresh:
                a[pl.ds(pl.multiple_of(k * chunk, chunk), chunk), :] = jnp.zeros((chunk, width), jnp.float32)
            return carry
        if fresh:
            lax.fori_loop(0, n_rows // chunk, clear, 0)
        for a in accs:
            a[pl.ds(n_rows, 8), :] = jnp.zeros((8, width), jnp.float32)
        if grad_ref is not None:
            cp_in.wait()

        for which, (idx, cnt, vals_ref, extra) in enumerate(work):
            per_list = vals_ref.shape[0] // idx.shape[0]

            def one_list(i, carry, which=which, idx=idx, cnt=cnt, vals_ref=vals_ref, extra=extra, per_list=per_list):
                def group(q, c2):
                    for u in range(8):
                        c = q * 8 + u
                        acc = accs[u % n_acc]
                        r = idx[i, c]
                        if which == 0:
                            acc[pl.ds(r, 1), :] += extra[i, c] * wide[pl.ds(i * per_list + c, 1), :]
                        else:
                            acc[pl.ds(r, 1), :] += vals_ref[pl.ds(extra[i, c], 1), :]
                    return c2
                return lax.fori_loop(0, (cnt[i] + 7) // 8, group, carry)
            lax.fori_loop(0, idx.shape[0], one_list, 0)

        piece = n_rows // 8

        def leave(k):
            sl = pl.ds(pl.multiple_of(k * piece, piece), piece)
            return pltpu.make_async_copy(accs[0].at[sl], out_ref.at[sl], out_sem.at[k])

        def finish(k, carry):
            if n_acc > 1:
                def merge(q, c2):
                    sl = pl.ds(pl.multiple_of(k * piece + q * cut, cut), cut)
                    tot = accs[0][sl, :]
                    for a in accs[1:]:
                        tot = tot + a[sl, :]
                    accs[0][sl, :] = tot
                    return c2
                lax.fori_loop(0, piece // cut, merge, 0)

            @pl.when(k > 0)
            def _():
                leave(k - 1).start()
            return carry
        lax.fori_loop(0, 8, finish, 0)
        leave(7).start()
        lax.fori_loop(0, 8, lambda k, c: (leave(k).wait(), c)[1], 0)

    return pl.pallas_call(
        kernel,
        out_shape=jax.ShapeDtypeStruct((n_rows, width), jnp.float32),
        in_specs=specs,
        out_specs=ANY,
        scratch_shapes=[pltpu.VMEM((n_full, width), jnp.float32)] * n_acc + [
            pltpu.VMEM(groups[0][2].shape, jnp.float32), pltpu.SemaphoreType.DMA, pltpu.SemaphoreType.DMA((8,))],
        compiler_params=pltpu.CompilerParams(vmem_limit_bytes=60 * 1024 * 1024),
    )(*flat)


def ranks(owner, n_row):
    n = owner.shape[0]
    hot = (owner[:, None] == jnp.arange(n_row)[None, :]).astype(jnp.bfloat16)
    pos = jnp.arange(n)
    before = (pos[:, None] > pos[None, :]).astype(jnp.bfloat16)
    earlier = jnp.dot(before, hot, preferred_element_type=jnp.float32)
    hot32 = hot.astype(jnp.float32)
    return jnp.sum(earlier * hot32, axis=1).astype(jnp.int32), jnp.sum(hot32, axis=0).astype(jnp.int32)


def to_slots(slot, vals, n_slots):
    hit = slot[:, None] == jnp.arange(n_slots)[None, :]
    return [jnp.sum(jnp.where(hit, v[:, None], jnp.zeros((), v.dtype)), axis=0) for v in vals]


def tile_rows(rows, n_row):
    padded = [jnp.pad(r, ((0, 0), (0, LANES - r.shape[1]))) for r in rows]
    padded += [jnp.zeros_like(padded[0])] * (8 - len(rows))
    return jnp.stack(padded, axis=1)


def solution(mesh):
    n_row, n_dp = mesh.shape["row"], mesh.shape["dp"]
    n_dev = n_row * n_dp
    side = round(n_row ** (1 / 3))

    def run_step(x_tok, w_up, w_down, item_table, cand_ids, log_q, targets):
        n_total = x_tok.shape[0]

        def device_step(x_loc, w_up, w_down, tab_loc, cand_ids, log_q, y_loc):
            rows_local, width = tab_loc.shape
            n_tok = y_loc.shape[0]
            n_cand = cand_ids.shape[0]
            row, dp = lax.axis_index("row"), lax.axis_index("dp")
            me = dp * n_row + row
            chunk = n_cand // n_dev
            f32, bf16 = jnp.float32, jnp.bfloat16
            n_ids = n_tok + chunk
            n_pad = -(-n_ids // LANES) * LANES

            my_cands = lax.dynamic_slice_in_dim(cand_ids, me * chunk, chunk)
            ids = jnp.concatenate([y_loc, my_cands])
            owner, local = ids // rows_local, ids % rows_local
            rank, per_owner = ranks(owner, n_row)
            most = jnp.max(per_owner)

            pre_act = jnp.dot(x_loc, w_up, preferred_element_type=f32)
            act_full, gelu_vjp = jax.vjp(jax.nn.gelu, pre_act)
            act_b = act_full.astype(bf16)
            hidden = jnp.dot(act_b, w_down, preferred_element_type=f32).astype(bf16)

            split = jnp.pad(jnp.stack([local // 128, local % 128], axis=1).astype(bf16), ((0, n_pad - n_ids), (0, LANES - 2)))
            carried = jnp.concatenate([jnp.pad(hidden, ((0, n_pad - n_tok), (0, 0))), split], axis=1)

            def pack_round(k):
                rel = rank - k * CAP
                hit = (rel >= 0) & (rel < CAP)
                slot = jnp.where(hit, owner * LANES + rel, -1)
                hid_out, want = pack(jnp.pad(slot, (0, n_pad - n_ids), constant_values=-1)[None, :], carried, n_row)
                return hit, owner * CAP + rel, hid_out, want

            def fetch_round(k):
                hit, at, hid_out, want = pack_round(k)
                lane = jnp.arange(LANES)[None, None, :]
                rows_in, most_all = fetch(n_row, n_dp, jnp.where(lane == LANES - 1, most, want), tab_loc)
                got = jnp.take(rows_in.reshape(n_row * CAP, width), at, axis=0, mode="clip")
                return hit, got, hid_out, want, most_all

            _, got, hid_out, want, most_dp = fetch_round(0)
            cand_rows, most_all = gather_cands(n_row, n_dp, got, n_tok, most_dp)
            most_all = most_all[0, LANES - 1]

            def fetch_more(carry):
                k, got, _ = carry
                hit, new, _, _, most = fetch_round(k)
                got = jnp.where(hit[:, None], new, got)
                return k + 1, got, gather_cands(n_row, n_dp, got, n_tok, most)[0]

            _, got, cand_rows = lax.while_loop(
                lambda c: c[0] * CAP < most_all, fetch_more, (jnp.int32(1), got, cand_rows))
            cand_rows = cand_rows.reshape(n_cand, width)

            cand_grad, grad_hid, dz_lanes, loss_part = softmax(
                n_total, cand_rows, hidden, got,
                jnp.broadcast_to(y_loc[:, None], (n_tok, LANES)), cand_ids[None, :], log_q[None, :])
            loss_sum = loss_part[0, 0]

            grad_down = jnp.einsum("tf,td->fd", act_b, grad_hid, preferred_element_type=f32)
            grad_act = jnp.einsum("td,fd->tf", grad_hid, w_down, preferred_element_type=f32)
            grad_pre = gelu_vjp(grad_act)[0].astype(bf16)
            grad_up = jnp.einsum("ti,tf->if", x_loc, grad_pre, preferred_element_type=f32)

            t_rank, t_owner = rank[:n_tok], owner[:n_tok]
            t_count = jnp.sum((t_owner[:, None] == jnp.arange(n_row)[None, :]).astype(jnp.int32), axis=0)
            c_rank, _ = ranks(owner[n_tok:], n_row)
            c_slot = owner[n_tok:] * chunk + c_rank
            c_count = per_owner - t_count
            c_row, c_pos = to_slots(c_slot, [(local[n_tok:] - rows_local).astype(f32), jnp.arange(chunk, dtype=f32)], n_row * chunk)
            c_row = (c_row + rows_local).reshape(n_row, chunk)
            c_pos = c_pos.reshape(n_row, chunk)
            half, z_y_x = chunk // 2, coords(row, side)
            first = []
            for part in range(2):
                a, b, c = order(part, *z_y_x)
                first.append((((part * n_dp + dp) * n_row + (a * side + b) * side + c) * half).astype(f32))
            c_pos = jnp.where(c_pos < half, first[0] + c_pos, first[1] + c_pos - half)

            def give(k, want):
                rel = t_rank - k * CAP
                slot = jnp.where((rel >= 0) & (rel < CAP), t_owner * LANES + rel, -1)
                now = jnp.clip(t_count - k * CAP, 0, CAP).astype(f32)
                counts = jnp.stack([now, c_count.astype(f32), jnp.full((n_row,), loss_sum)], axis=1)
                base = tile_rows([want[:, 0, :CAP].astype(f32), jnp.zeros((n_row, LANES), f32), c_row, c_pos, counts], n_row)
                return place(base, jnp.broadcast_to(slot[:, None], (n_tok, LANES)), dz_lanes)

            to_int = lambda v: v.astype(jnp.int32)

            def token_group(hid_in, meta_in):
                return to_int(meta_in[:, 0, :CAP]), to_int(meta_in[:, 4, 0]), hid_in.reshape(n_dev * CAP, width), meta_in[:, 1, :CAP]

            blocks = w_up.shape[1] // LANES
            up_shape = (n_dev // blocks, w_up.shape[0] * blocks // n_dev, blocks, LANES)
            rest = jnp.concatenate([
                grad_up.reshape(up_shape).transpose(0, 2, 1, 3).reshape(n_dp, n_row, up_shape[1], width),
                grad_down.reshape(n_dp, n_row, -1, width)], axis=2)
            parts = core_sum(side, cand_grad.reshape(n_dp, n_row, 2, half, width), rest)
            g0, g1, g2, hid_in, meta_in = axis_sum(side, n_dp, parts, [hid_out, give(0, want)])
            cand_sums, g2, hid_in, meta_in = core_swap(n_dp, (g0, g1), (g2,), (hid_in,), (meta_in,))
            hid_in, meta_in = hid_in.reshape(n_dev, CAP, width), meta_in.reshape(n_dev, 8, LANES)
            cand_sums = cand_sums.reshape(n_cand, width)
            rest = jnp.transpose(g2[0], (0, 1, 3, 2, 4, 5)).reshape(n_dev, -1, width)
            grad_up = rest[:, :up_shape[1]].reshape(up_shape[0], blocks, up_shape[1], LANES).transpose(0, 2, 1, 3).reshape(w_up.shape)
            grad_down = rest[:, up_shape[1]:].reshape(w_down.shape)

            grad = add_rows(rows_local, [
                token_group(hid_in, meta_in),
                (to_int(meta_in[:, 2, :chunk]), to_int(meta_in[:, 4, 1]), cand_sums, to_int(meta_in[:, 3, :chunk]))])

            def give_more(carry):
                k, grad = carry
                _, _, hid_more, want_more = pack_round(k)
                return k + 1, add_rows(rows_local, [token_group(*exchange(n_row, n_dp, True, hid_more, give(k, want_more)))], grad, 1)

            _, grad = lax.while_loop(lambda c: c[0] * CAP < most_all, give_more, (jnp.int32(1), grad))
            return jnp.sum(meta_in[:, 4, 2]) / n_total, grad, grad_up, grad_down

        return jax.shard_map(
            device_step,
            mesh=mesh,
            in_specs=(P(ALL_AXES, None), P(), P(), P("row", None), P(), P(), P(ALL_AXES)),
            out_specs=(P(), P("row", None), P(), P()),
            check_vma=False,
        )(x_tok, w_up, w_down, item_table, cand_ids, log_q, targets)

    return run_step
```
